32 devices in a mesh: ty: 2 (over core), tx: 4 (over z), pos: 4 (over y, x).
Axes of the slice: x: 2, y: 2, z: 4, core: 2. Of those that a mesh axis runs over, the one named last changes fastest.
Arguments:
- object_field: float32 [2, 2, 512, 1024], P(None, None, ('ty', 'pos'), 'tx'), may hold values from -6 to 6
- momentum: float32 [2, 2, 512, 1024], P(None, None, ('ty', 'pos'), 'tx'), may hold values from -12 to 12
- measured: float32 [2, 4, 4, 256, 256], P('ty', 'tx', 'pos'), may hold values from 0 to 2
- illumination: float32 [2, 256, 256], replicated, may hold values from -6 to 6
- slab_phase: float32 [256, 256], replicated, may hold values from -3.140625 to 3.140625
- offsets: int32 [2, 4, 4, 2], P('ty', 'tx'), may hold values from 0 to 128, as said below
- entry_counts: int32 [2, 4], P('ty', 'tx'), may hold values from 1 to 2, as said below
Outputs:
- new_object: float32 [2, 2, 512, 1024], P(None, None, ('ty', 'pos'), 'tx')
- new_momentum: float32 [2, 2, 512, 1024], P(None, None, ('ty', 'pos'), 'tx')
- amplitudes: float32 [2, 4, 4, 256, 256], P('ty', 'tx', 'pos')
The draws below stay inside these ranges and needn't reach their ends.
Inputs may be any that keep to these rules, and one draw needn't show every extreme that they name: offsets[a, b, k] is the corner of a window of 256 x 256 cells, counted from the corner of tile (a, b) widened by 64 cells on every side. Tile (a, b) uses the first entry_counts[a, b] slots of its list; some tile uses exactly 2 slots in every draw.
All inputs are finite; a program needn't handle non-finite values.
Results may differ from the reference program's by a relative error of at most 0.0003.
Values sent between devices are 32-bit elements; how exact they have to be, the bound alone decides.
No kernel may reach another device: no remote copies, remote signals or barrier semaphores. Data moves between devices by JAX's collectives and lax.ppermute only.
A program may use at most 64 MiB of HBM per device.

```python
import math
import jax
import jax.numpy as jnp
from jax import lax

W = 256
TILE = 256
MARGIN = 64
LIST = 4
TROWS = 2
TCOLS = 4
NYO = 512
NXO = 1024


def draw_offsets(key, part):
    return jax.random.randint(key, (TROWS, TCOLS, LIST, 2), 0, TILE + 2 * MARGIN - W + 1, dtype=jnp.int32)


def draw_entry_counts(key, part):
    tiles = TROWS * TCOLS
    drawn = jax.random.randint(jax.random.fold_in(key, 11), (tiles,), max(1, LIST // 4), LIST // 2 + 1, dtype=jnp.int32)
    chosen = jax.random.randint(jax.random.fold_in(key, 12), (), 0, tiles, dtype=jnp.int32)
    flat_index = jnp.arange(tiles, dtype=jnp.int32)
    return jnp.where(flat_index == chosen, LIST // 2, drawn).reshape(TROWS, TCOLS).astype(jnp.int32)


def levels(own_key, extent, shards, smallest, largest):
    gain, own = 1.0, jax.random.fold_in(own_key, 6)
    for dim, shards_of in shards:
        steps = jnp.exp(jax.random.uniform(jax.random.fold_in(own, dim), (shards_of,), jnp.float32, smallest / len(shards), largest / len(shards)))
        gain = gain * jnp.repeat(steps, extent[dim] // shards_of).reshape([-1 if axis == dim else 1 for axis in range(len(extent))])
    return gain


def bell_draw(own_key, extent, spread, limit, pieces=(), held_as=jnp.bfloat16):
    factor_of = levels(own_key, extent, pieces, -0.22, 0.18) if pieces else 1.0
    values = jax.random.normal(own_key, extent, jnp.float32) * spread * factor_of
    return jnp.minimum(jnp.maximum(values, -limit), limit).astype(held_as)


def setup_inputs(seed: int = 0) -> dict:
    key_of = jax.random.split(jax.random.key(seed), 8)
    return {
        "object_field": bell_draw(key_of[0], (2, 2, NYO, NXO), 1.0, 6.0, ((2, 8), (3, 4)), jnp.float32),
        "momentum": bell_draw(key_of[1], (2, 2, NYO, NXO), 2.0, 12.0, ((2, 8), (3, 4)), jnp.float32),
        "measured": jnp.clip(2.0 * jax.random.uniform(key_of[2], (TROWS, TCOLS, LIST, W, W), jnp.float32) ** levels(key_of[2], (TROWS, TCOLS, LIST, W, W), ((0, 2), (1, 4), (2, 4)), -0.2, 0.2), 0.0, 2.0),
        "illumination": bell_draw(key_of[3], (2, W, W), 1.0, 6.0, (), jnp.float32),
        "slab_phase": jnp.clip(jax.random.uniform(key_of[4], (W, W), jnp.float32, -3.140625, 3.140625), -3.140625, 3.140625),
        "offsets": draw_offsets(jax.random.fold_in(key_of[7], 71), 0),
        "entry_counts": draw_entry_counts(jax.random.fold_in(key_of[7], 71), 0),
    }


HIGHEST = lax.Precision.HIGHEST
magnitude_floor = 0.5
momentum_rate = 0.9
step_length = 0.05

def tables(length):
    indices = jnp.arange(length, dtype=jnp.int32)
    product = indices[:, None] * indices[None, :] % length
    angles = product.astype(jnp.float32) * (2.0 * math.pi / length)
    factor = 1.0 / math.sqrt(length)
    return (jnp.cos(angles) * factor, jnp.sin(angles) * factor)

def matmul(left, right):
    return jnp.dot(left, right, precision=HIGHEST)

def transform(real_part, imag_part, cosine, sine_table, inverse):
    factor = 1.0 if inverse else -1.0
    right_real = matmul(real_part, cosine) - factor * matmul(imag_part, sine_table)
    right_imag = matmul(imag_part, cosine) + factor * matmul(real_part, sine_table)
    left_real = matmul(cosine, right_real) - factor * matmul(sine_table, right_imag)
    left_imag = matmul(cosine, right_imag) + factor * matmul(sine_table, right_real)
    return (left_real, left_imag)

def complex_product(first_real, first_imag, second_real, second_imag):
    return (first_real * second_real - first_imag * second_imag, first_real * second_imag + first_imag * second_real)

def forward_window(window, illumination, slab_real, slab_imag, cosine, sine_table):
    entering = complex_product(illumination[0], illumination[1], window[0], window[1])
    spectrum = transform(entering[0], entering[1], cosine, sine_table, False)
    spectrum = complex_product(spectrum[0], spectrum[1], slab_real, slab_imag)
    between = transform(spectrum[0], spectrum[1], cosine, sine_table, True)
    leaving = complex_product(between[0], between[1], window[2], window[3])
    farfield = transform(leaving[0], leaving[1], cosine, sine_table, False)
    return (between, farfield)

def window_gradient(window, measured_window, illumination, slab_real, slab_imag, cosine, sine_table):
    between, farfield = forward_window(window, illumination, slab_real, slab_imag, cosine, sine_table)
    magnitude = jnp.sqrt(farfield[0] * farfield[0] + farfield[1] * farfield[1])
    keeping = 1.0 - measured_window / jnp.maximum(magnitude, magnitude_floor)
    backward = transform(farfield[0] * keeping, farfield[1] * keeping, cosine, sine_table, True)
    grad_second = complex_product(between[0], -between[1], backward[0], backward[1])
    toward = complex_product(window[2], -window[3], backward[0], backward[1])
    spectrum = transform(toward[0], toward[1], cosine, sine_table, False)
    spectrum = complex_product(spectrum[0], spectrum[1], slab_real, -slab_imag)
    incoming = transform(spectrum[0], spectrum[1], cosine, sine_table, True)
    grad_first = complex_product(illumination[0], -illumination[1], incoming[0], incoming[1])
    return jnp.stack([grad_first[0], grad_first[1], grad_second[0], grad_second[1]])

def reference(object_field, momentum, measured, illumination, slab_phase, offsets, entry_counts):
    cosine, sine_table = tables(W)
    slab_real = jnp.cos(slab_phase)
    slab_imag = jnp.sin(slab_phase)
    layers = object_field.reshape(4, NYO, NXO)
    widths = ((0, 0), (MARGIN, MARGIN), (MARGIN, MARGIN))
    padded = jnp.pad(layers, widths)
    total = TROWS * TCOLS * LIST
    zero = jnp.zeros((), jnp.int32)

    def locate(entry):
        tile_index = entry // LIST
        within = entry % LIST
        tile_row = tile_index // TCOLS
        tile_col = tile_index % TCOLS
        place = offsets[tile_row, tile_col, within]
        row_start = (tile_row * TILE + place[0]).astype(jnp.int32)
        col_start = (tile_col * TILE + place[1]).astype(jnp.int32)
        live = (within < entry_counts[tile_row, tile_col]).astype(jnp.float32)
        return (tile_row, tile_col, within, row_start, col_start, live)

    def accumulate(gradient, entry):
        tile_row, tile_col, within, row_start, col_start, live = locate(entry)
        window = lax.dynamic_slice(padded, (zero, row_start, col_start), (4, W, W))
        term = window_gradient(window, measured[tile_row, tile_col, within], illumination, slab_real, slab_imag, cosine, sine_table) * live
        current = lax.dynamic_slice(gradient, (zero, row_start, col_start), (4, W, W))
        return (lax.dynamic_update_slice(gradient, current + term, (zero, row_start, col_start)), live)
    entries = jnp.arange(total, dtype=jnp.int32)
    gradient = lax.scan(accumulate, jnp.zeros(padded.shape, jnp.float32), entries)[0]
    interior = gradient[:, MARGIN:MARGIN + NYO, MARGIN:MARGIN + NXO]
    velocity = momentum_rate * momentum.reshape(4, NYO, NXO) + interior
    updated = layers - step_length * velocity
    refreshed = jnp.pad(updated, widths)

    def predict(entry):
        tile_row, tile_col, within, row_start, col_start, live = locate(entry)
        window = lax.dynamic_slice(refreshed, (zero, row_start, col_start), (4, W, W))
        farfield = forward_window(window, illumination, slab_real, slab_imag, cosine, sine_table)[1]
        return jnp.sqrt(farfield[0] * farfield[0] + farfield[1] * farfield[1]) * live
    amplitudes = lax.map(predict, entries).reshape(TROWS, TCOLS, LIST, W, W)
    return (updated.reshape(2, 2, NYO, NXO), velocity.reshape(2, 2, NYO, NXO), amplitudes)
```

```python
import math

import jax
import jax.numpy as jnp
import numpy as np
from jax import lax
from jax.experimental import pallas as pl
from jax.experimental.pallas import tpu as pltpu
from jax.sharding import PartitionSpec as P

magnitude_floor = 0.5
momentum_rate = 0.9
step_length = 0.05
F32 = jnp.float32
BF16 = jnp.bfloat16


def vmem():
    return pl.BlockSpec(memory_space=pltpu.VMEM)


def smem():
    return pl.BlockSpec(memory_space=pltpu.SMEM)


def call(body, outs, args, scalars=0, scratch=(), name=None):
    specs = [smem()] * scalars + [vmem()] * (len(args) - scalars)
    return pl.pallas_call(
        body,
        out_shape=tuple(jax.ShapeDtypeStruct(s, F32) for s in outs),
        in_specs=specs,
        out_specs=tuple(vmem() for _ in outs),
        scratch_shapes=list(scratch),
        name=name,
        compiler_params=pltpu.CompilerParams(vmem_limit_bytes=56 * 1024 * 1024),
    )(*args)


def split_table(values):
    high = values.astype(jnp.bfloat16)
    low = (values - high.astype(np.float64)).astype(jnp.bfloat16)
    return high, low


def dft_tables(length):
    index = np.arange(length)
    angles = (index[:, None] * index[None, :] % length) * (2.0 * math.pi / length)
    cosine, sine = np.cos(angles) / math.sqrt(length), np.sin(angles) / math.sqrt(length)
    parts = [part for t in (cosine, cosine + sine, cosine - sine) for part in split_table(t)]
    return np.stack(parts)


def iota(shape, dim):
    return lax.broadcasted_iota(jnp.int32, shape, dim)


def split(value):
    high = value.astype(BF16)
    return high, (value - high.astype(F32)).astype(BF16)


def dot(left, right):
    return jnp.dot(left, right, preferred_element_type=F32)


def mul3(left, right):
    return dot(left[0], right[0]) + dot(left[0], right[1]) + dot(left[1], right[0])


def transform(real, imag, tab, inverse):
    cos = (tab[0], tab[1])
    plus, minus = ((tab[4], tab[5]), (tab[2], tab[3])) if inverse else ((tab[2], tab[3]), (tab[4], tab[5]))
    both = mul3(split(real + imag), cos)
    right_imag = both - mul3(split(real), plus)
    right_real = both - mul3(split(imag), minus)
    both = mul3(cos, split(right_real + right_imag))
    left_imag = both - mul3(plus, split(right_real))
    left_real = both - mul3(minus, split(right_imag))
    return left_real, left_imag


def cmul(ar, ai, br, bi):
    return ar * br - ai * bi, ar * bi + ai * br


class Layout:
    def __init__(self, object_field, illumination, offsets):
        self.n = lax.axis_size("pos")
        self.ntx = lax.axis_size("tx")
        self.nty = lax.axis_size("ty")
        self.h = object_field.shape[2]
        self.t = object_field.shape[3]
        self.m = illumination.shape[-1] // 4
        self.slots = offsets.shape[2]
        self.half = self.n // 2
        assert self.nty == 2 and self.slots == self.n and self.n & (self.n - 1) == 0
        assert self.t == illumination.shape[-1] == self.n * self.h == 4 * self.m

    def window_of(self, device, row, home):
        return device if home else device - row * self.half

    def holds(self, device, row, home):
        return 0 <= self.window_of(device, row, home) < self.half

    def inward(self, s, home):
        n = self.n
        return [(a * n + p, a * n + (p ^ s)) for a in range(2) for p in range(n) if self.holds(p ^ s, a, home)]

    def outward(self, s):
        return [(d, o) for o, d in self.inward(s, False)]


def complete(pairs, n):
    sources, targets = {x for x, _ in pairs}, {y for _, y in pairs}
    other = lambda x: (x + n) % (2 * n)
    extra = [(x, other(x)) for x in range(2 * n) if x not in sources and other(x) not in targets]
    return pairs + extra if len(pairs) + len(extra) == 2 * n else pairs


def where_am_i():
    return lax.axis_index("ty"), lax.axis_index("tx"), lax.axis_index("pos")


def masks(place_ref, k, a, p, lay):
    h, t, m = lay.h, lay.t, lay.m
    k = jnp.clip(k, 0, lay.slots - 1)
    top = place_ref[0, 0, k, 0] - m
    left = place_ref[0, 0, k, 1] - m
    rows = iota((h, t), 0) + p * h
    cols = iota((h, t), 1)
    above = rows >= top + t
    below = rows < top
    outside = above | below
    partner = (above & (a == 1)) | (below & (a == 0))
    halo = (cols >= left + t) | (cols < left)
    return outside, partner, halo


def pack_blocks(place_ref, own, own_halo, prt, prt_halo, out_refs, lay, home):
    a, _, p = where_am_i()
    for s in range(lay.n):
        k = lay.window_of(p ^ s, a, home)
        outside, partner, halo = masks(place_ref, k, a, p, lay)
        for c in range(4):
            mine = jnp.where(halo, spread(own_halo[c], lay), own[c])
            theirs = jnp.where(halo, spread(prt_halo[c], lay), prt[c])
            out_refs[s][c] = jnp.where(partner, theirs, jnp.where(outside, 0.0, mine))


def spread(halo, lay):
    return halo if lay.t == 2 * lay.m else jnp.concatenate([halo, halo], axis=1)


def roll_half(x, lay):
    return pltpu.roll(x, lay.m, 1)


def kernel_strips(lay):
    t, m = lay.t, lay.m

    def body(own_ref, prt_ref, out_ref):
        a = lax.axis_index("ty")
        low = iota((lay.h, 2 * m), 1) < m
        for c in range(4):
            for row in (0, 1):

                @pl.when(a == row)
                def _(c=c, row=row):
                    cut = slice(t - 2 * m, t) if row == 0 else slice(0, 2 * m)
                    first, second = (own_ref, prt_ref) if row == 0 else (prt_ref, own_ref)
                    x0, x1 = first[c, :, cut], roll_half(second[c, :, cut], lay)
                    out_ref[c] = jnp.where(low, x1, x0) if row == 0 else jnp.where(low, x0, x1)

    return body


def kernel_pack(lay):
    m = lay.m

    def body(place_ref, own_ref, prt_ref, mine_ref, theirs_ref, *outs):
        a, b, _ = where_am_i()
        blocks, own_halo_ref, prt_halo_ref = outs[: lay.n], outs[lay.n], outs[lay.n + 1]
        low = iota((lay.h, 2 * m), 1) < m
        keep = jnp.where(low, (b < lay.ntx - 1).astype(F32), (b > 0).astype(F32))
        for c in range(4):
            from_left = jnp.where(a == 0, mine_ref[c], theirs_ref[c])
            from_right = jnp.where(a == 0, theirs_ref[c], mine_ref[c])
            halo0 = jnp.where(low, from_right, from_left)
            halo1 = jnp.where(low, roll_half(from_right, lay), roll_half(from_left, lay))
            own_halo_ref[c] = jnp.where(keep > 0, jnp.where(a == 0, halo0, halo1), 0.0)
            prt_halo_ref[c] = jnp.where(keep > 0, jnp.where(a == 0, halo1, halo0), 0.0)
        pack_blocks(place_ref, own_ref, own_halo_ref, prt_ref, prt_halo_ref, blocks, lay, False)

    return body


def kernel_probe(lay):
    def body(place_ref, light_ref, out_ref):
        a, _, p = where_am_i()
        for i, home in enumerate((False, True)):
            k = jnp.clip(lay.window_of(p, a, home), 0, lay.slots - 1)
            down = (place_ref[0, 0, k, 0] + (lay.t - lay.m)) % lay.t
            along = (place_ref[0, 0, k, 1] + (lay.t - lay.m)) % lay.t
            for c in range(2):
                out_ref[i, c] = pltpu.roll(pltpu.roll(light_ref[c], down, 0), along, 1)

    return body


def assemble(blocks, window_ref, lay):
    p = lax.axis_index("pos")
    for s in range(lay.n):
        start = pl.multiple_of((p ^ s) * lay.h, lay.h)
        for c in range(4):
            window_ref[c, pl.ds(start, lay.h), :] = blocks[s][c]


def forward(window_ref, light_ref, which, slab_ref, tab):
    o1r, o1i, o2r, o2i = (window_ref[c] for c in range(4))
    er, ei = cmul(light_ref[which, 0], light_ref[which, 1], o1r, o1i)
    sr, si = transform(er, ei, tab, False)
    sr, si = cmul(sr, si, slab_ref[0], slab_ref[1])
    br, bi = transform(sr, si, tab, True)
    lr, li = cmul(br, bi, o2r, o2i)
    return br, bi, transform(lr, li, tab, False)


def kernel_gradient(lay):
    def body(count_ref, *refs):
        n = lay.n
        blocks, (light_ref, slab_ref, tab, meas_ref, moved_ref) = refs[:n], refs[n : n + 5]
        outs, window_ref = refs[n + 5 : 2 * n + 5], refs[2 * n + 5]
        a, _, p = where_am_i()
        k = lay.window_of(p, a, False)

        @pl.when((k >= 0) & (k < count_ref[0, 0]))
        def _():
            assemble(blocks, window_ref, lay)
            br, bi, (fr, fi) = forward(window_ref, light_ref, 0, slab_ref, tab)
            seen = jnp.where(a == 0, meas_ref[0, 0, 0], moved_ref[0, 0, 0])
            keeping = 1.0 - seen / jnp.maximum(jnp.sqrt(fr * fr + fi * fi), magnitude_floor)
            kr, ki = transform(fr * keeping, fi * keeping, tab, True)
            g2r, g2i = cmul(br, -bi, kr, ki)
            tr, ti = cmul(window_ref[2], -window_ref[3], kr, ki)
            window_ref[2] = g2r
            window_ref[3] = g2i
            sr, si = transform(tr, ti, tab, False)
            sr, si = cmul(sr, si, slab_ref[0], -slab_ref[1])
            ir, ii = transform(sr, si, tab, True)
            g1r, g1i = cmul(light_ref[0, 0], -light_ref[0, 1], ir, ii)
            window_ref[0] = g1r
            window_ref[1] = g1i
            for s in range(n):
                start = pl.multiple_of((p ^ s) * lay.h, lay.h)
                for c in range(4):
                    outs[s][c] = window_ref[c, pl.ds(start, lay.h), :]

    return body


def kernel_collect(lay):
    t, m = lay.t, lay.m

    def body(place_ref, count_ref, *refs):
        n = lay.n
        blocks, mom_ref = refs[:n], refs[n]
        own_ref, halo_ref = refs[n + 1 :]
        a, _, p = where_am_i()
        low = iota((lay.h, 2 * m), 1) < m
        own_ref[0] = momentum_rate * mom_ref[...]
        own_ref[1] = jnp.zeros(own_ref.shape[1:], F32)
        halo_ref[...] = jnp.zeros(halo_ref.shape, F32)
        for s in range(n):
            k = lay.window_of(p ^ s, a, False)

            @pl.when((k >= 0) & (k < count_ref[0, 0]))
            def _(s=s, k=k):
                outside, partner, halo = masks(place_ref, k, a, p, lay)
                for c in range(4):
                    g = blocks[s][c]
                    for i, rows in enumerate((~outside, partner)):
                        own_ref[i, c] += jnp.where(rows & ~halo, g, 0.0)
                        x = jnp.where(rows & halo, g, 0.0)
                        halo_ref[i, c] += jnp.where(low, x[:, : 2 * m], x[:, t - 2 * m :])

    return body


def kernel_strips_back(lay):
    t, m = lay.t, lay.m

    def body(own_ref, halo_ref, their_own_ref, their_halo_ref, sum_ref, halo_sum_ref, out_ref):
        a = lax.axis_index("ty")
        low = iota((lay.h, 2 * m), 1) < m
        for c in range(4):
            for i in range(2):
                sum_ref[i, c] = own_ref[i, c] + their_own_ref[1 - i, c]
                halo_sum_ref[i, c] = halo_ref[i, c] + their_halo_ref[1 - i, c]
        for row in (0, 1):

            @pl.when(a == row)
            def _(row=row):
                for tile in range(2):
                    i = tile ^ row
                    for c in range(4):
                        halo = halo_sum_ref[i, c]
                        if row == 0:
                            out_ref[tile, c] = jnp.where(low, halo, sum_ref[i, c, :, t - 2 * m :])
                        else:
                            out_ref[tile, c] = jnp.where(low, sum_ref[i, c, :, : 2 * m], halo)

    return body


def kernel_update(lay):
    t, m = lay.t, lay.m

    def body(place_ref, obj_ref, prt_ref, obj_halo_ref, prt_halo_ref, sum_ref, halo_sum_ref, mine_ref, theirs_ref, *outs):
        n = lay.n
        new_ref, vel_ref, blocks, prt_new, own_halo, prt_halo = outs[0], outs[1], outs[2 : n + 2], *outs[n + 2 :]
        a, b, _ = where_am_i()
        low = iota((lay.h, 2 * m), 1) < m
        not_first, not_last = b > 0, b < lay.ntx - 1
        keep = (low & not_last) | (~low & not_first)
        for i in range(2):
            tile = a if i == 0 else 1 - a
            for c in range(4):
                mine, theirs = mine_ref[tile, c], theirs_ref[tile, c]
                from_left = jnp.where(not_first, jnp.where(a == 0, mine, theirs), 0.0)
                from_right = jnp.where(not_last, jnp.where(a == 0, theirs, mine), 0.0)
                v = sum_ref[i, c] + jnp.concatenate(
                    [jnp.where(low, from_left, 0.0), jnp.where(low, 0.0, from_right)], axis=1
                )
                hv = halo_sum_ref[i, c] + jnp.where(low, from_right, from_left)
                obj, halo = (obj_ref, obj_halo_ref) if i == 0 else (prt_ref, prt_halo_ref)
                new, new_halo = (new_ref, own_halo) if i == 0 else (prt_new, prt_halo)
                if i == 0:
                    vel_ref[c] = v
                new[c] = obj[c] - step_length * v
                new_halo[c] = jnp.where(keep, halo[c] - step_length * hv, 0.0)
        pack_blocks(place_ref, new_ref, own_halo, prt_new, prt_halo, blocks, lay, True)

    return body


def kernel_predict(lay):
    def body(count_ref, *refs):
        n = lay.n
        blocks, (light_ref, slab_ref, tab), out_ref, window_ref = refs[:n], refs[n : n + 3], refs[n + 3], refs[n + 4]
        p = lax.axis_index("pos")

        @pl.when(p < count_ref[0, 0])
        def _():
            assemble(blocks, window_ref, lay)
            _, _, (fr, fi) = forward(window_ref, light_ref, 1, slab_ref, tab)
            out_ref[0, 0, 0] = jnp.sqrt(fr * fr + fi * fi)

        @pl.when(p >= count_ref[0, 0])
        def _():
            out_ref[...] = jnp.zeros(out_ref.shape, F32)

    return body


def shards(object_field, momentum, measured, illumination, slab_phase, offsets, entry_counts):
    lay = Layout(object_field, illumination, offsets)
    n, h, t, m = lay.n, lay.h, lay.t, lay.m
    own = object_field.reshape(4, h, t)
    velocity_old = momentum.reshape(4, h, t)
    block, halo_shape = (4, h, t), (4, h, 2 * m)
    cores = lambda x: lax.ppermute(x, "ty", [(0, 1), (1, 0)])
    ring = [((a * lay.ntx + b), a * lay.ntx + (b + 1 - 2 * a) % lay.ntx) for a in range(2) for b in range(lay.ntx)]
    columns = lambda x: lax.ppermute(x, ("ty", "tx"), ring)
    send = lambda x, pairs: lax.ppermute(x, ("ty", "pos"), complete(pairs, n))

    moved = lax.ppermute(measured, "pos", [(p, p ^ lay.half) for p in range(n)])
    tab = jnp.asarray(dft_tables(t))
    slab = jnp.stack([jnp.cos(slab_phase), jnp.sin(slab_phase)])
    (light,) = call(kernel_probe(lay), [(2, 2, t, t)], [offsets, illumination], 1, name="probe_move")

    partner = cores(own)
    (strips,) = call(kernel_strips(lay), [halo_shape], [own, partner], name="strips")
    strips = columns(strips)
    strips_other = cores(strips)
    *blocks, own_halo, partner_halo = call(
        kernel_pack(lay),
        [block] * n + [halo_shape] * 2,
        [offsets, own, partner, strips, strips_other],
        1,
        name="pack",
    )
    received = [blocks[0]] + [send(blocks[s], lay.inward(s, False)) for s in range(1, n)]
    window = pltpu.VMEM((4, t, t), F32)
    terms = call(
        kernel_gradient(lay),
        [block] * n,
        [entry_counts, *received, light, slab, tab, measured, moved],
        1,
        [window],
        name="gradient",
    )
    parts = [terms[0]] + [send(terms[s], lay.outward(s)) for s in range(1, n)]
    sums, halos = call(
        kernel_collect(lay),
        [(2, *block), (2, *halo_shape)],
        [offsets, entry_counts, *parts, velocity_old],
        2,
        name="collect",
    )
    sums, halos, strips = call(
        kernel_strips_back(lay),
        [(2, *block), (2, *halo_shape), (2, *halo_shape)],
        [sums, halos, cores(sums), cores(halos)],
        name="strips_back",
    )
    strips = columns(strips)
    updated, velocity, *rest = call(
        kernel_update(lay),
        [block] * (n + 3) + [halo_shape] * 2,
        [offsets, own, partner, own_halo, partner_halo, sums, halos, strips, cores(strips)],
        1,
        name="update",
    )
    blocks = rest[:n]
    received = [blocks[0]] + [send(blocks[s], lay.inward(s, True)) for s in range(1, n)]
    (amplitudes,) = call(
        kernel_predict(lay),
        [measured.shape],
        [entry_counts, *received, light, slab, tab],
        1,
        [window],
        name="predict",
    )
    return (
        updated.reshape(object_field.shape),
        velocity.reshape(momentum.shape),
        amplitudes,
    )


def solution(mesh):
    placed = (
        P(None, None, ("ty", "pos"), "tx"),
        P(None, None, ("ty", "pos"), "tx"),
        P("ty", "tx", "pos", None, None),
        P(),
        P(),
        P("ty", "tx", None, None),
        P("ty", "tx"),
    )
    return jax.shard_map(
        shards,
        mesh=mesh,
        in_specs=placed,
        out_specs=(
            P(None, None, ("ty", "pos"), "tx"),
            P(None, None, ("ty", "pos"), "tx"),
            P("ty", "tx", "pos", None, None),
        ),
        check_vma=False,
    )
```

```python
import math

import jax
import jax.numpy as jnp
import numpy as np
from jax import lax
from jax.experimental import pallas as pl
from jax.experimental.pallas import tpu as pltpu
from jax.sharding import PartitionSpec as P


magnitude_floor = 0.5
momentum_rate = 0.9
step_length = 0.05
F32 = jnp.float32
BF16 = jnp.bfloat16


def vmem():
    return pl.BlockSpec(memory_space=pltpu.VMEM)


def smem():
    return pl.BlockSpec(memory_space=pltpu.SMEM)


def call(body, outs, args, scalars=0, scratch=(), limit=8, last=False):
    specs = [smem()] * scalars + [vmem()] * (len(args) - scalars)
    placed = [pltpu.with_memory_space_constraint(x, pltpu.VMEM) for x in args[scalars:]]
    return pl.pallas_call(
        body,
        out_shape=tuple((jax.ShapeDtypeStruct if last else pltpu.VMEM)(s, F32) for s in outs),
        in_specs=specs,
        out_specs=tuple(vmem() for _ in outs),
        scratch_shapes=list(scratch),
        compiler_params=pltpu.CompilerParams(vmem_limit_bytes=limit * 1024 * 1024),
    )(*args[:scalars], *placed)


def split_table(values):
    high = values.astype(jnp.bfloat16)
    low = (values - high.astype(np.float64)).astype(jnp.bfloat16)
    return high, low


def dft_tables(length):
    index = np.arange(length)
    angles = (index[:, None] * index[None, :] % length) * (2.0 * math.pi / length)
    cosine, sine = np.cos(angles) / math.sqrt(length), np.sin(angles) / math.sqrt(length)
    parts = [part for t in (cosine, cosine + sine, cosine - sine) for part in split_table(t)]
    return np.stack(parts)


def iota(shape, dim):
    return lax.broadcasted_iota(jnp.int32, shape, dim)


def split(value):
    high = value.astype(BF16)
    return high, (value - high.astype(F32)).astype(BF16)


def dot(left, right):
    return jnp.dot(left, right, preferred_element_type=F32)


def mul3(left, right):
    return dot(left[0], right[0]) + dot(left[0], right[1]) + dot(left[1], right[0])


def transform(real, imag, tab, inverse):
    cos = (tab[0], tab[1])
    plus, minus = ((tab[4], tab[5]), (tab[2], tab[3])) if inverse else ((tab[2], tab[3]), (tab[4], tab[5]))
    both = mul3(split(real + imag), cos)
    right_imag = both - mul3(split(real), plus)
    right_real = both - mul3(split(imag), minus)
    both = mul3(cos, split(right_real + right_imag))
    left_imag = both - mul3(plus, split(right_real))
    left_real = both - mul3(minus, split(right_imag))
    return left_real, left_imag


def cmul(ar, ai, br, bi):
    return ar * br - ai * bi, ar * bi + ai * br


class Layout:
    def __init__(self, object_field, illumination, offsets):
        self.n = lax.axis_size("pos")
        self.ntx = lax.axis_size("tx")
        self.nty = lax.axis_size("ty")
        self.h = object_field.shape[2]
        self.t = object_field.shape[3]
        self.m = illumination.shape[-1] // 4
        self.slots = offsets.shape[2]
        self.half = self.n // 2
        assert self.nty == 2 and self.slots == self.n and self.n & (self.n - 1) == 0
        assert self.t == illumination.shape[-1] == self.n * self.h == 4 * self.m

    def window_of(self, device, row, home):
        return device if home else device - row * self.half

    def holds(self, device, row, home):
        return 0 <= self.window_of(device, row, home) < self.half

    def inward(self, s, home):
        n = self.n
        return [(a * n + p, a * n + (p ^ s)) for a in range(2) for p in range(n) if self.holds(p ^ s, a, home)]

    def outward(self, s):
        return [(d, o) for o, d in self.inward(s, False)]


def complete(pairs, n):
    sources, targets = {x for x, _ in pairs}, {y for _, y in pairs}
    other = lambda x: (x + n) % (2 * n)
    extra = [(x, other(x)) for x in range(2 * n) if x not in sources and other(x) not in targets]
    return pairs + extra if len(pairs) + len(extra) == 2 * n else pairs


def where_am_i():
    return lax.axis_index("ty"), lax.axis_index("tx"), lax.axis_index("pos")


def masks(place_ref, k, a, p, lay):
    h, t, m = lay.h, lay.t, lay.m
    k = jnp.clip(k, 0, lay.slots - 1)
    top = place_ref[0, 0, 0, k] - m
    left = place_ref[0, 0, 1, k] - m
    rows = iota((h, t), 0) + p * h
    cols = iota((h, t), 1)
    above = rows >= top + t
    below = rows < top
    outside = above | below
    partner = (above & (a == 1)) | (below & (a == 0))
    halo = (cols >= left + t) | (cols < left)
    return outside, partner, halo


def pack_blocks(place_ref, own, own_halo, prt, prt_halo, out_refs, lay, home):
    a, _, p = where_am_i()
    for s in range(lay.n):
        k = lay.window_of(p ^ s, a, home)
        outside, partner, halo = masks(place_ref, k, a, p, lay)
        for c in range(4):
            mine = jnp.where(halo, spread(own_halo[c], lay), own[c])
            theirs = jnp.where(halo, spread(prt_halo[c], lay), prt[c])
            out_refs[s][c] = jnp.where(partner, theirs, jnp.where(outside, 0.0, mine))


def spread(halo, lay):
    return halo if lay.t == 2 * lay.m else jnp.concatenate([halo, halo], axis=1)


def roll_half(x, lay):
    return pltpu.roll(x, lay.m, 1)


def kernel_strips(lay):
    t, m = lay.t, lay.m

    def body(own_ref, prt_ref, out_ref):
        a = lax.axis_index("ty")
        low = iota((lay.h, 2 * m), 1) < m
        for c in range(4):
            for row in (0, 1):

                @pl.when(a == row)
                def _(c=c, row=row):
                    cut = slice(t - 2 * m, t) if row == 0 else slice(0, 2 * m)
                    first, second = (own_ref, prt_ref) if row == 0 else (prt_ref, own_ref)
                    x0, x1 = first[c, :, cut], roll_half(second[c, :, cut], lay)
                    out_ref[c] = jnp.where(low, x1, x0) if row == 0 else jnp.where(low, x0, x1)

    return body


def kernel_pack(lay):
    m = lay.m

    def body(place_ref, own_ref, prt_ref, mine_ref, theirs_ref, *outs):
        a, b, _ = where_am_i()
        blocks, own_halo_ref, prt_halo_ref = outs[: lay.n], outs[lay.n], outs[lay.n + 1]
        low = iota((lay.h, 2 * m), 1) < m
        keep = jnp.where(low, (b < lay.ntx - 1).astype(F32), (b > 0).astype(F32))
        for c in range(4):
            from_left = jnp.where(a == 0, mine_ref[c], theirs_ref[c])
            from_right = jnp.where(a == 0, theirs_ref[c], mine_ref[c])
            halo0 = jnp.where(low, from_right, from_left)
            halo1 = jnp.where(low, roll_half(from_right, lay), roll_half(from_left, lay))
            own_halo_ref[c] = jnp.where(keep > 0, jnp.where(a == 0, halo0, halo1), 0.0)
            prt_halo_ref[c] = jnp.where(keep > 0, jnp.where(a == 0, halo1, halo0), 0.0)
        pack_blocks(place_ref, own_ref, own_halo_ref, prt_ref, prt_halo_ref, blocks, lay, False)

    return body


def kernel_probe(lay):
    def body(place_ref, light_ref, phase_ref, out_ref, slab_ref):
        a, _, p = where_am_i()
        slab_ref[0] = jnp.cos(phase_ref[...])
        slab_ref[1] = jnp.sin(phase_ref[...])
        for i, home in enumerate((False, True)):
            k = jnp.clip(lay.window_of(p, a, home), 0, lay.slots - 1)
            down = (place_ref[0, 0, 0, k] + (lay.t - lay.m)) % lay.t
            along = (place_ref[0, 0, 1, k] + (lay.t - lay.m)) % lay.t
            for c in range(2):
                out_ref[i, c] = pltpu.roll(pltpu.roll(light_ref[c], down, 0), along, 1)

    return body


def assemble(blocks, window_ref, lay):
    p = lax.axis_index("pos")
    for s in range(lay.n):
        start = pl.multiple_of((p ^ s) * lay.h, lay.h)
        for c in range(4):
            window_ref[c, pl.ds(start, lay.h), :] = blocks[s][c]


def forward(window_ref, light_ref, which, slab_ref, tab):
    o1r, o1i, o2r, o2i = (window_ref[c] for c in range(4))
    er, ei = cmul(light_ref[which, 0], light_ref[which, 1], o1r, o1i)
    sr, si = transform(er, ei, tab, False)
    sr, si = cmul(sr, si, slab_ref[0], slab_ref[1])
    br, bi = transform(sr, si, tab, True)
    lr, li = cmul(br, bi, o2r, o2i)
    return br, bi, transform(lr, li, tab, False)


def kernel_gradient(lay):
    def body(count_ref, *refs):
        n = lay.n
        blocks, (light_ref, slab_ref, tab, meas_ref, moved_ref) = refs[:n], refs[n : n + 5]
        outs, window_ref = refs[n + 5 : 2 * n + 5], refs[2 * n + 5]
        a, _, p = where_am_i()
        k = lay.window_of(p, a, False)

        @pl.when((k >= 0) & (k < count_ref[0, 0]))
        def _():
            assemble(blocks, window_ref, lay)
            br, bi, (fr, fi) = forward(window_ref, light_ref, 0, slab_ref, tab)
            seen = jnp.where(a == 0, meas_ref[0, 0, 0], moved_ref[0, 0, 0])
            keeping = 1.0 - seen / jnp.maximum(jnp.sqrt(fr * fr + fi * fi), magnitude_floor)
            kr, ki = transform(fr * keeping, fi * keeping, tab, True)
            g2r, g2i = cmul(br, -bi, kr, ki)
            tr, ti = cmul(window_ref[2], -window_ref[3], kr, ki)
            window_ref[2] = g2r
            window_ref[3] = g2i
            sr, si = transform(tr, ti, tab, False)
            sr, si = cmul(sr, si, slab_ref[0], -slab_ref[1])
            ir, ii = transform(sr, si, tab, True)
            g1r, g1i = cmul(light_ref[0, 0], -light_ref[0, 1], ir, ii)
            window_ref[0] = g1r
            window_ref[1] = g1i
            for s in range(n):
                start = pl.multiple_of((p ^ s) * lay.h, lay.h)
                for c in range(4):
                    outs[s][c] = window_ref[c, pl.ds(start, lay.h), :]

    return body


def kernel_collect(lay):
    t, m = lay.t, lay.m

    def body(place_ref, count_ref, *refs):
        n = lay.n
        blocks, mom_ref = refs[:n], refs[n]
        own_ref, halo_ref = refs[n + 1 :]
        a, _, p = where_am_i()
        low = iota((lay.h, 2 * m), 1) < m
        own_ref[0] = momentum_rate * mom_ref[...]
        own_ref[1] = jnp.zeros(own_ref.shape[1:], F32)
        halo_ref[...] = jnp.zeros(halo_ref.shape, F32)
        for s in range(n):
            k = lay.window_of(p ^ s, a, False)

            @pl.when((k >= 0) & (k < count_ref[0, 0]))
            def _(s=s, k=k):
                outside, partner, halo = masks(place_ref, k, a, p, lay)
                for c in range(4):
                    g = blocks[s][c]
                    for i, rows in enumerate((~outside, partner)):
                        own_ref[i, c] += jnp.where(rows & ~halo, g, 0.0)
                        x = jnp.where(rows & halo, g, 0.0)
                        halo_ref[i, c] += jnp.where(low, x[:, : 2 * m], x[:, t - 2 * m :])

    return body


def kernel_strips_back(lay):
    t, m = lay.t, lay.m

    def body(own_ref, halo_ref, their_own_ref, their_halo_ref, sum_ref, halo_sum_ref, out_ref):
        a = lax.axis_index("ty")
        low = iota((lay.h, 2 * m), 1) < m
        for c in range(4):
            for i in range(2):
                sum_ref[i, c] = own_ref[i, c] + their_own_ref[1 - i, c]
                halo_sum_ref[i, c] = halo_ref[i, c] + their_halo_ref[1 - i, c]
        for row in (0, 1):

            @pl.when(a == row)
            def _(row=row):
                for tile in range(2):
                    i = tile ^ row
                    for c in range(4):
                        halo = halo_sum_ref[i, c]
                        if row == 0:
                            out_ref[tile, c] = jnp.where(low, halo, sum_ref[i, c, :, t - 2 * m :])
                        else:
                            out_ref[tile, c] = jnp.where(low, sum_ref[i, c, :, : 2 * m], halo)

    return body


def kernel_update(lay):
    m = lay.m

    def body(place_ref, obj_ref, prt_ref, obj_halo_ref, prt_halo_ref, sum_ref, halo_sum_ref, mine_ref, theirs_ref, *outs):
        n = lay.n
        new_ref, vel_ref, blocks, prt_new, own_halo, prt_halo = outs[0], outs[1], outs[2 : n + 2], *outs[n + 2 :]
        a, b, _ = where_am_i()
        low = iota((lay.h, 2 * m), 1) < m
        not_first, not_last = b > 0, b < lay.ntx - 1
        keep = (low & not_last) | (~low & not_first)
        for i in range(2):
            tile = a if i == 0 else 1 - a
            for c in range(4):
                mine, theirs = mine_ref[tile, c], theirs_ref[tile, c]
                from_left = jnp.where(not_first, jnp.where(a == 0, mine, theirs), 0.0)
                from_right = jnp.where(not_last, jnp.where(a == 0, theirs, mine), 0.0)
                v = sum_ref[i, c] + jnp.concatenate(
                    [jnp.where(low, from_left, 0.0), jnp.where(low, 0.0, from_right)], axis=1
                )
                hv = halo_sum_ref[i, c] + jnp.where(low, from_right, from_left)
                obj, halo = (obj_ref, obj_halo_ref) if i == 0 else (prt_ref, prt_halo_ref)
                new, new_halo = (new_ref, own_halo) if i == 0 else (prt_new, prt_halo)
                if i == 0:
                    vel_ref[c] = v
                new[c] = obj[c] - step_length * v
                new_halo[c] = jnp.where(keep, halo[c] - step_length * hv, 0.0)
        pack_blocks(place_ref, new_ref, own_halo, prt_new, prt_halo, blocks, lay, True)

    return body


def kernel_predict(lay):
    def body(count_ref, *refs):
        n = lay.n
        blocks, (light_ref, slab_ref, tab), out_ref, window_ref = refs[:n], refs[n : n + 3], refs[n + 3], refs[n + 4]
        p = lax.axis_index("pos")

        @pl.when(p < count_ref[0, 0])
        def _():
            assemble(blocks, window_ref, lay)
            _, _, (fr, fi) = forward(window_ref, light_ref, 1, slab_ref, tab)
            out_ref[0, 0, 0] = jnp.sqrt(fr * fr + fi * fi)

        @pl.when(p >= count_ref[0, 0])
        def _():
            out_ref[...] = jnp.zeros(out_ref.shape, F32)

    return body


def iteration(object_field, momentum, measured, illumination, slab_phase, offsets, entry_counts):
    lay = Layout(object_field, illumination, offsets)
    n, h, t, m = lay.n, lay.h, lay.t, lay.m
    own = object_field.reshape(4, h, t)
    offsets = offsets.transpose(0, 1, 3, 2)
    velocity_old = momentum.reshape(4, h, t)
    block, halo_shape = (4, h, t), (4, h, 2 * m)
    cores = lambda x: lax.ppermute(x, "ty", [(0, 1), (1, 0)])
    ntx = lay.ntx
    shift = [(b, b + 1) for b in range(ntx - 1)] + [(ntx - 1, 2 * ntx - 1)]
    shift += [(ntx + b + 1, ntx + b) for b in range(ntx - 1)] + [(ntx, 0)]
    columns = lambda x: lax.ppermute(x, ("ty", "tx"), shift)

    def exchange(values, pairs_of):
        got = {0: values[0]}
        for s in [*range(lay.half, n), *range(1, lay.half)]:
            got[s] = lax.ppermute(values[s], ("ty", "pos"), complete(pairs_of(s), n))
        return [got[s] for s in range(n)]

    moved = lax.ppermute(measured, "pos", [(p, p ^ lay.half) for p in range(n)])
    tab = jnp.asarray(dft_tables(t))
    light, slab = call(kernel_probe(lay), [(2, 2, t, t), (2, t, t)], [offsets, illumination, slab_phase], 1)

    partner = cores(own)
    (strips,) = call(kernel_strips(lay), [halo_shape], [own, partner])
    strips = columns(strips)
    strips_other = cores(strips)
    *blocks, own_halo, partner_halo = call(
        kernel_pack(lay), [block] * n + [halo_shape] * 2, [offsets, own, partner, strips, strips_other], 1
    )
    received = exchange(blocks, lambda s: lay.inward(s, False))
    window = pltpu.VMEM((4, t, t), F32)
    terms = call(
        kernel_gradient(lay),
        [block] * n,
        [entry_counts, *received, light, slab, tab, measured, moved],
        1,
        [window],
        limit=24,
    )
    parts = exchange(terms, lay.outward)
    sums, halos = call(
        kernel_collect(lay), [(2, *block), (2, *halo_shape)], [offsets, entry_counts, *parts, velocity_old], 2
    )
    sums, halos, strips = call(
        kernel_strips_back(lay),
        [(2, *block), (2, *halo_shape), (2, *halo_shape)],
        [sums, halos, cores(sums), cores(halos)],
    )
    strips = columns(strips)
    updated, velocity, *rest = call(
        kernel_update(lay),
        [block] * (n + 3) + [halo_shape] * 2,
        [offsets, own, partner, own_halo, partner_halo, sums, halos, strips, cores(strips)],
        1,
    )
    blocks = rest[:n]
    received = exchange(blocks, lambda s: lay.inward(s, True))
    (amplitudes,) = call(
        kernel_predict(lay),
        [measured.shape],
        [entry_counts, *received, light, slab, tab],
        1,
        [window],
        limit=24,
        last=True,
    )
    return (
        updated.reshape(object_field.shape),
        velocity.reshape(momentum.shape),
        amplitudes,
    )


def solution(mesh):
    placed = (
        P(None, None, ("ty", "pos"), "tx"),
        P(None, None, ("ty", "pos"), "tx"),
        P("ty", "tx", "pos", None, None),
        P(),
        P(),
        P("ty", "tx", None, None),
        P("ty", "tx"),
    )
    return jax.shard_map(
        iteration,
        mesh=mesh,
        in_specs=placed,
        out_specs=(
            P(None, None, ("ty", "pos"), "tx"),
            P(None, None, ("ty", "pos"), "tx"),
            P("ty", "tx", "pos", None, None),
        ),
        check_vma=False,
    )
```

```python
import math

import jax
import jax.numpy as jnp
import numpy as np
from jax import lax
from jax.experimental import pallas as pl
from jax.experimental.pallas import tpu as pltpu
from jax.sharding import PartitionSpec as P


magnitude_floor = 0.5
momentum_rate = 0.9
step_length = 0.05
F32 = jnp.float32
BF16 = jnp.bfloat16


def vmem():
    return pl.BlockSpec(memory_space=pltpu.VMEM)


def smem():
    return pl.BlockSpec(memory_space=pltpu.SMEM)


def call(body, outs, args, scalars=0, scratch=(), limit=8, last=False):
    specs = [smem()] * scalars + [vmem()] * (len(args) - scalars)
    placed = [pltpu.with_memory_space_constraint(x, pltpu.VMEM) for x in args[scalars:]]
    return pl.pallas_call(
        body,
        out_shape=tuple((jax.ShapeDtypeStruct if last else pltpu.VMEM)(s, F32) for s in outs),
        in_specs=specs,
        out_specs=tuple(vmem() for _ in outs),
        scratch_shapes=list(scratch),
        compiler_params=pltpu.CompilerParams(vmem_limit_bytes=limit * 1024 * 1024),
    )(*args[:scalars], *placed)


def split_table(values):
    high = values.astype(jnp.bfloat16)
    low = (values - high.astype(np.float64)).astype(jnp.bfloat16)
    return high, low


def dft_tables(length):
    index = np.arange(length)
    angles = (index[:, None] * index[None, :] % length) * (2.0 * math.pi / length)
    cosine, sine = np.cos(angles) / math.sqrt(length), np.sin(angles) / math.sqrt(length)
    parts = [part for t in (cosine, cosine + sine, cosine - sine) for part in split_table(t)]
    return np.stack(parts)


def iota(shape, dim):
    return lax.broadcasted_iota(jnp.int32, shape, dim)


def split(value):
    high = value.astype(BF16)
    return high, (value - high.astype(F32)).astype(BF16)


def dot(left, right):
    return jnp.dot(left, right, preferred_element_type=F32)


def mul3(left, right):
    return dot(left[0], right[0]) + dot(left[0], right[1]) + dot(left[1], right[0])


def transform(real, imag, tab, inverse):
    cos = (tab[0], tab[1])
    plus, minus = ((tab[4], tab[5]), (tab[2], tab[3])) if inverse else ((tab[2], tab[3]), (tab[4], tab[5]))
    both = mul3(split(real + imag), cos)
    right_imag = both - mul3(split(real), plus)
    right_real = both - mul3(split(imag), minus)
    both = mul3(cos, split(right_real + right_imag))
    left_imag = both - mul3(plus, split(right_real))
    left_real = both - mul3(minus, split(right_imag))
    return left_real, left_imag


def cmul(ar, ai, br, bi):
    return ar * br - ai * bi, ar * bi + ai * br


class Layout:
    def __init__(self, object_field, illumination, offsets):
        self.n = lax.axis_size("pos")
        self.ntx = lax.axis_size("tx")
        self.nty = lax.axis_size("ty")
        self.h = object_field.shape[2]
        self.t = object_field.shape[3]
        self.m = illumination.shape[-1] // 4
        self.slots = offsets.shape[2]
        self.half = self.n // 2
        assert self.nty == 2 and self.slots == self.n and self.n & (self.n - 1) == 0
        assert self.t == illumination.shape[-1] == self.n * self.h == 4 * self.m

    def window_of(self, device, row, home):
        return device if home else device - row * self.half

    def holds(self, device, row, home):
        return 0 <= self.window_of(device, row, home) < self.half

    def inward(self, s, home):
        n = self.n
        return [(a * n + p, a * n + (p ^ s)) for a in range(2) for p in range(n) if self.holds(p ^ s, a, home)]

    def outward(self, s):
        return [(d, o) for o, d in self.inward(s, False)]


def complete(pairs, n):
    sources, targets = {x for x, _ in pairs}, {y for _, y in pairs}
    other = lambda x: (x + n) % (2 * n)
    extra = [(x, other(x)) for x in range(2 * n) if x not in sources and other(x) not in targets]
    return pairs + extra if len(pairs) + len(extra) == 2 * n else pairs


def where_am_i():
    return lax.axis_index("ty"), lax.axis_index("tx"), lax.axis_index("pos")


def masks(place_ref, k, a, p, lay):
    h, t, m = lay.h, lay.t, lay.m
    k = jnp.clip(k, 0, lay.slots - 1)
    top = place_ref[0, 0, 0, k] - m
    left = place_ref[0, 0, 1, k] - m
    rows = iota((h, t), 0) + p * h
    cols = iota((h, t), 1)
    above = rows >= top + t
    below = rows < top
    outside = above | below
    partner = (above & (a == 1)) | (below & (a == 0))
    halo = (cols >= left + t) | (cols < left)
    return outside, partner, halo


def pack_blocks(place_ref, own, own_halo, prt, prt_halo, out_refs, lay, home):
    a, _, p = where_am_i()
    for s in range(lay.n):
        k = lay.window_of(p ^ s, a, home)
        outside, partner, halo = masks(place_ref, k, a, p, lay)
        for c in range(4):
            mine = jnp.where(halo, spread(own_halo[c], lay), own[c])
            theirs = jnp.where(halo, spread(prt_halo[c], lay), prt[c])
            value = jnp.where(partner, theirs, jnp.where(outside, 0.0, mine))
            if home:
                out_refs[c // 2 * lay.n + s][c % 2] = value
            else:
                out_refs[s][c] = value


def spread(halo, lay):
    return halo if lay.t == 2 * lay.m else jnp.concatenate([halo, halo], axis=1)


def roll_half(x, lay):
    return pltpu.roll(x, lay.m, 1)


def kernel_strips(lay):
    t, m = lay.t, lay.m

    def body(own_ref, prt_ref, out_ref):
        a = lax.axis_index("ty")
        low = iota((lay.h, 2 * m), 1) < m
        for c in range(4):
            for row in (0, 1):

                @pl.when(a == row)
                def _(c=c, row=row):
                    cut = slice(t - 2 * m, t) if row == 0 else slice(0, 2 * m)
                    first, second = (own_ref, prt_ref) if row == 0 else (prt_ref, own_ref)
                    x0, x1 = first[c, :, cut], roll_half(second[c, :, cut], lay)
                    out_ref[c] = jnp.where(low, x1, x0) if row == 0 else jnp.where(low, x0, x1)

    return body


def kernel_pack(lay):
    m = lay.m

    def body(place_ref, own_ref, prt_ref, mine_ref, theirs_ref, *outs):
        a, b, _ = where_am_i()
        blocks, own_halo_ref, prt_halo_ref = outs[: lay.n], outs[lay.n], outs[lay.n + 1]
        low = iota((lay.h, 2 * m), 1) < m
        keep = jnp.where(low, (b < lay.ntx - 1).astype(F32), (b > 0).astype(F32))
        for c in range(4):
            from_left = jnp.where(a == 0, mine_ref[c], theirs_ref[c])
            from_right = jnp.where(a == 0, theirs_ref[c], mine_ref[c])
            halo0 = jnp.where(low, from_right, from_left)
            halo1 = jnp.where(low, roll_half(from_right, lay), roll_half(from_left, lay))
            own_halo_ref[c] = jnp.where(keep > 0, jnp.where(a == 0, halo0, halo1), 0.0)
            prt_halo_ref[c] = jnp.where(keep > 0, jnp.where(a == 0, halo1, halo0), 0.0)
        pack_blocks(place_ref, own_ref, own_halo_ref, prt_ref, prt_halo_ref, blocks, lay, False)

    return body


def load(*arrays):
    count = len(arrays)

    def body(*refs):
        sources, targets, sems = refs[:count], refs[count : 2 * count], refs[2 * count]
        copies = [pltpu.make_async_copy(x, y, sems.at[i]) for i, (x, y) in enumerate(zip(sources, targets))]
        for copy in copies:
            copy.start()
        for copy in copies:
            copy.wait()

    return pl.pallas_call(
        body,
        out_shape=tuple(pltpu.VMEM(x.shape, x.dtype) for x in arrays),
        in_specs=[pl.BlockSpec(memory_space=pl.ANY)] * count,
        out_specs=tuple(vmem() for _ in arrays),
        scratch_shapes=[pltpu.SemaphoreType.DMA((count,))],
        name="load_kernel",
        compiler_params=pltpu.CompilerParams(vmem_limit_bytes=2 * 1024 * 1024),
    )(*[pltpu.with_memory_space_constraint(x, pltpu.HBM) for x in arrays])


def kernel_slab(phase_ref, slab_ref):
    slab_ref[0] = jnp.cos(phase_ref[...])
    slab_ref[1] = jnp.sin(phase_ref[...])


def kernel_probe(lay):
    def body(place_ref, light_ref, out_ref):
        a, _, p = where_am_i()
        for i, home in enumerate((False, True)):
            k = jnp.clip(lay.window_of(p, a, home), 0, lay.slots - 1)
            down = (place_ref[0, 0, 0, k] + (lay.t - lay.m)) % lay.t
            along = (place_ref[0, 0, 1, k] + (lay.t - lay.m)) % lay.t
            for c in range(2):
                out_ref[i, c] = pltpu.roll(pltpu.roll(light_ref[c], down, 0), along, 1)

    return body


def assemble(blocks, window_ref, lay):
    p = lax.axis_index("pos")
    for s in range(lay.n):
        start = pl.multiple_of((p ^ s) * lay.h, lay.h)
        for c in range(window_ref.shape[0]):
            window_ref[c, pl.ds(start, lay.h), :] = blocks[s][c]


def propagate(o1r, o1i, light_ref, which, slab_ref, tab):
    er, ei = cmul(light_ref[which, 0], light_ref[which, 1], o1r, o1i)
    sr, si = transform(er, ei, tab, False)
    sr, si = cmul(sr, si, slab_ref[0], slab_ref[1])
    return transform(sr, si, tab, True)


def kernel_gradient(lay):
    def body(count_ref, *refs):
        n = lay.n
        blocks, (light_ref, slab_ref, tab, meas_ref, moved_ref) = refs[:n], refs[n : n + 5]
        outs, window_ref = refs[n + 5 : 2 * n + 5], refs[2 * n + 5]
        a, _, p = where_am_i()
        k = lay.window_of(p, a, False)

        @pl.when((k >= 0) & (k < count_ref[0, 0]))
        def _():
            assemble(blocks, window_ref, lay)
            br, bi = propagate(window_ref[0], window_ref[1], light_ref, 0, slab_ref, tab)
            lr, li = cmul(br, bi, window_ref[2], window_ref[3])
            fr, fi = transform(lr, li, tab, False)
            seen = jnp.where(a == 0, meas_ref[0, 0, 0], moved_ref[0, 0, 0])
            keeping = 1.0 - seen / jnp.maximum(jnp.sqrt(fr * fr + fi * fi), magnitude_floor)
            kr, ki = transform(fr * keeping, fi * keeping, tab, True)
            g2r, g2i = cmul(br, -bi, kr, ki)
            tr, ti = cmul(window_ref[2], -window_ref[3], kr, ki)
            window_ref[2] = g2r
            window_ref[3] = g2i
            sr, si = transform(tr, ti, tab, False)
            sr, si = cmul(sr, si, slab_ref[0], -slab_ref[1])
            ir, ii = transform(sr, si, tab, True)
            g1r, g1i = cmul(light_ref[0, 0], -light_ref[0, 1], ir, ii)
            window_ref[0] = g1r
            window_ref[1] = g1i
            for s in range(n):
                start = pl.multiple_of((p ^ s) * lay.h, lay.h)
                for c in range(4):
                    outs[s][c] = window_ref[c, pl.ds(start, lay.h), :]

    return body


def kernel_collect(lay):
    t, m = lay.t, lay.m

    def body(place_ref, count_ref, *refs):
        n = lay.n
        blocks, mom_ref = refs[:n], refs[n]
        own_ref, halo_ref = refs[n + 1 :]
        a, _, p = where_am_i()
        low = iota((lay.h, 2 * m), 1) < m
        own_ref[0] = momentum_rate * mom_ref[...]
        own_ref[1] = jnp.zeros(own_ref.shape[1:], F32)
        halo_ref[...] = jnp.zeros(halo_ref.shape, F32)
        for s in range(n):
            k = lay.window_of(p ^ s, a, False)

            @pl.when((k >= 0) & (k < count_ref[0, 0]))
            def _(s=s, k=k):
                outside, partner, halo = masks(place_ref, k, a, p, lay)
                for c in range(4):
                    g = blocks[s][c]
                    for i, rows in enumerate((~outside, partner)):
                        own_ref[i, c] += jnp.where(rows & ~halo, g, 0.0)
                        x = jnp.where(rows & halo, g, 0.0)
                        halo_ref[i, c] += jnp.where(low, x[:, : 2 * m], x[:, t - 2 * m :])

    return body


def kernel_strips_back(lay):
    t, m = lay.t, lay.m

    def body(own_ref, halo_ref, their_own_ref, their_halo_ref, sum_ref, halo_sum_ref, out_ref):
        a = lax.axis_index("ty")
        low = iota((lay.h, 2 * m), 1) < m
        for c in range(4):
            for i in range(2):
                sum_ref[i, c] = own_ref[i, c] + their_own_ref[1 - i, c]
                halo_sum_ref[i, c] = halo_ref[i, c] + their_halo_ref[1 - i, c]
        for row in (0, 1):

            @pl.when(a == row)
            def _(row=row):
                for tile in range(2):
                    i = tile ^ row
                    for c in range(4):
                        halo = halo_sum_ref[i, c]
                        if row == 0:
                            out_ref[tile, c] = jnp.where(low, halo, sum_ref[i, c, :, t - 2 * m :])
                        else:
                            out_ref[tile, c] = jnp.where(low, sum_ref[i, c, :, : 2 * m], halo)

    return body


def kernel_update(lay):
    m = lay.m

    def body(place_ref, obj_ref, prt_ref, obj_halo_ref, prt_halo_ref, sum_ref, halo_sum_ref, mine_ref, theirs_ref, *outs):
        n = lay.n
        new_ref, vel_ref, *blocks = outs[: 2 * n + 2]
        prt_new, own_halo, prt_halo = outs[2 * n + 2 :]
        a, b, _ = where_am_i()
        low = iota((lay.h, 2 * m), 1) < m
        not_first, not_last = b > 0, b < lay.ntx - 1
        keep = (low & not_last) | (~low & not_first)
        for i in range(2):
            tile = a if i == 0 else 1 - a
            for c in range(4):
                mine, theirs = mine_ref[tile, c], theirs_ref[tile, c]
                from_left = jnp.where(not_first, jnp.where(a == 0, mine, theirs), 0.0)
                from_right = jnp.where(not_last, jnp.where(a == 0, theirs, mine), 0.0)
                v = sum_ref[i, c] + jnp.concatenate(
                    [jnp.where(low, from_left, 0.0), jnp.where(low, 0.0, from_right)], axis=1
                )
                hv = halo_sum_ref[i, c] + jnp.where(low, from_right, from_left)
                obj, halo = (obj_ref, obj_halo_ref) if i == 0 else (prt_ref, prt_halo_ref)
                new, new_halo = (new_ref, own_halo) if i == 0 else (prt_new, prt_halo)
                if i == 0:
                    vel_ref[c] = v
                new[c] = obj[c] - step_length * v
                new_halo[c] = jnp.where(keep, halo[c] - step_length * hv, 0.0)
        pack_blocks(place_ref, new_ref, own_halo, prt_new, prt_halo, blocks, lay, True)

    return body


def kernel_between(lay):
    def body(count_ref, *refs):
        n = lay.n
        blocks, (light_ref, slab_ref, tab), out_ref, window_ref = refs[:n], refs[n : n + 3], refs[n + 3], refs[n + 4]

        @pl.when(lax.axis_index("pos") < count_ref[0, 0])
        def _():
            assemble(blocks, window_ref, lay)
            out_ref[0], out_ref[1] = propagate(window_ref[0], window_ref[1], light_ref, 1, slab_ref, tab)

    return body


def kernel_predict(lay):
    def body(count_ref, *refs):
        n = lay.n
        blocks, (between_ref, tab), out_ref, window_ref = refs[:n], refs[n : n + 2], refs[n + 2], refs[n + 3]
        live = lax.axis_index("pos") < count_ref[0, 0]

        @pl.when(live)
        def _():
            assemble(blocks, window_ref, lay)
            lr, li = cmul(between_ref[0], between_ref[1], window_ref[0], window_ref[1])
            fr, fi = transform(lr, li, tab, False)
            out_ref[0, 0, 0] = jnp.sqrt(fr * fr + fi * fi)

        @pl.when(jnp.logical_not(live))
        def _():
            out_ref[...] = jnp.zeros(out_ref.shape, F32)

    return body


def iteration(object_field, momentum, measured, illumination, slab_phase, offsets, entry_counts):
    lay = Layout(object_field, illumination, offsets)
    n, h, t, m = lay.n, lay.h, lay.t, lay.m
    own = object_field.reshape(4, h, t)
    offsets = offsets.transpose(0, 1, 3, 2)
    velocity_old = momentum.reshape(4, h, t)
    block, halo_shape = (4, h, t), (4, h, 2 * m)
    tab = jnp.asarray(dft_tables(t))
    cores = lambda x: lax.ppermute(x, "ty", [(0, 1), (1, 0)])
    partner = cores(own)
    own, velocity_old, measured, illumination, slab_phase, tab = load(
        own, velocity_old, measured, illumination, slab_phase, tab
    )
    ntx = lay.ntx
    shift = [(b, b + 1) for b in range(ntx - 1)] + [(ntx - 1, 2 * ntx - 1)]
    shift += [(ntx + b + 1, ntx + b) for b in range(ntx - 1)] + [(ntx, 0)]
    columns = lambda x: lax.ppermute(x, ("ty", "tx"), shift)

    def exchange(values, pairs_of):
        got = [values[0]]
        for s in range(1, n):
            got.append(lax.ppermute(values[s], ("ty", "pos"), complete(pairs_of(s), n)))
        return got

    moved = lax.ppermute(measured, "pos", [(p, p ^ lay.half) for p in range(n)])
    (slab,) = call(kernel_slab, [(2, t, t)], [slab_phase])
    (light,) = call(kernel_probe(lay), [(2, 2, t, t)], [offsets, illumination], 1)

    (strips,) = call(kernel_strips(lay), [halo_shape], [own, partner])
    strips = columns(strips)
    strips_other = cores(strips)
    *blocks, own_halo, partner_halo = call(
        kernel_pack(lay), [block] * n + [halo_shape] * 2, [offsets, own, partner, strips, strips_other], 1
    )
    received = exchange(blocks, lambda s: lay.inward(s, False))
    window = pltpu.VMEM((4, t, t), F32)
    terms = call(
        kernel_gradient(lay),
        [block] * n,
        [entry_counts, *received, light, slab, tab, measured, moved],
        1,
        [window],
        limit=24,
    )
    parts = exchange(terms, lay.outward)
    sums, halos = call(
        kernel_collect(lay), [(2, *block), (2, *halo_shape)], [offsets, entry_counts, *parts, velocity_old], 2
    )
    sums, halos, strips = call(
        kernel_strips_back(lay),
        [(2, *block), (2, *halo_shape), (2, *halo_shape)],
        [sums, halos, cores(sums), cores(halos)],
    )
    strips = columns(strips)
    updated, velocity, *rest = call(
        kernel_update(lay),
        [block] * 2 + [(2, h, t)] * (2 * n),
        [offsets, own, partner, own_halo, partner_halo, sums, halos, strips, cores(strips)],
        1,
        [pltpu.VMEM(block, F32), pltpu.VMEM(halo_shape, F32), pltpu.VMEM(halo_shape, F32)],
    )
    first = exchange(rest[:n], lambda s: lay.inward(s, True))
    second = exchange(rest[n : 2 * n], lambda s: lay.inward(s, True))
    half_window = pltpu.VMEM((2, t, t), F32)
    (between,) = call(
        kernel_between(lay), [(2, t, t)], [entry_counts, *first, light, slab, tab], 1, [half_window], limit=24
    )
    (amplitudes,) = call(
        kernel_predict(lay),
        [measured.shape],
        [entry_counts, *second, between, tab],
        1,
        [half_window],
        limit=24,
        last=True,
    )
    return (
        updated.reshape(object_field.shape),
        velocity.reshape(momentum.shape),
        amplitudes,
    )


def solution(mesh):
    placed = (
        P(None, None, ("ty", "pos"), "tx"),
        P(None, None, ("ty", "pos"), "tx"),
        P("ty", "tx", "pos", None, None),
        P(),
        P(),
        P("ty", "tx", None, None),
        P("ty", "tx"),
    )
    return jax.shard_map(
        iteration,
        mesh=mesh,
        in_specs=placed,
        out_specs=(
            P(None, None, ("ty", "pos"), "tx"),
            P(None, None, ("ty", "pos"), "tx"),
            P("ty", "tx", "pos", None, None),
        ),
        check_vma=False,
    )
```

```python
import math

import jax
import jax.numpy as jnp
import numpy as np
from jax import lax
from jax.experimental import pallas as pl
from jax.experimental.pallas import tpu as pltpu
from jax.sharding import PartitionSpec as P


magnitude_floor = 0.5
momentum_rate = 0.9
step_length = 0.05
F32 = jnp.float32
BF16 = jnp.bfloat16


def vmem():
    return pl.BlockSpec(memory_space=pltpu.VMEM)


def smem():
    return pl.BlockSpec(memory_space=pltpu.SMEM)


def call(body, outs, args, scalars=0, scratch=(), limit=8, last=False):
    specs = [smem()] * scalars + [vmem()] * (len(args) - scalars)
    placed = [pltpu.with_memory_space_constraint(x, pltpu.VMEM) for x in args[scalars:]]
    return pl.pallas_call(
        body,
        out_shape=tuple((jax.ShapeDtypeStruct if last else pltpu.VMEM)(s, F32) for s in outs),
        in_specs=specs,
        out_specs=tuple(vmem() for _ in outs),
        scratch_shapes=list(scratch),
        compiler_params=pltpu.CompilerParams(vmem_limit_bytes=limit * 1024 * 1024),
    )(*args[:scalars], *placed)


def split_table(values):
    high = values.astype(jnp.bfloat16)
    low = (values - high.astype(np.float64)).astype(jnp.bfloat16)
    return high, low


def dft_tables(length):
    index = np.arange(length)
    angles = (index[:, None] * index[None, :] % length) * (2.0 * math.pi / length)
    cosine, sine = np.cos(angles) / math.sqrt(length), np.sin(angles) / math.sqrt(length)
    parts = [part for t in (cosine, cosine + sine, cosine - sine) for part in split_table(t)]
    return np.stack(parts)


def iota(shape, dim):
    return lax.broadcasted_iota(jnp.int32, shape, dim)


def split(value):
    high = value.astype(BF16)
    return high, (value - high.astype(F32)).astype(BF16)


def dot(left, right):
    return jnp.dot(left, right, preferred_element_type=F32)


def mul3(left, right):
    return dot(left[0], right[0]) + dot(left[0], right[1]) + dot(left[1], right[0])


def transform(real, imag, tab, inverse):
    cos = (tab[0], tab[1])
    plus, minus = ((tab[4], tab[5]), (tab[2], tab[3])) if inverse else ((tab[2], tab[3]), (tab[4], tab[5]))
    both = mul3(split(real + imag), cos)
    right_imag = both - mul3(split(real), plus)
    right_real = both - mul3(split(imag), minus)
    both = mul3(cos, split(right_real + right_imag))
    left_imag = both - mul3(plus, split(right_real))
    left_real = both - mul3(minus, split(right_imag))
    return left_real, left_imag


def cmul(ar, ai, br, bi):
    return ar * br - ai * bi, ar * bi + ai * br


class Layout:
    def __init__(self, object_field, illumination, offsets):
        self.n = lax.axis_size("pos")
        self.ntx = lax.axis_size("tx")
        self.nty = lax.axis_size("ty")
        self.h = object_field.shape[2]
        self.t = object_field.shape[3]
        self.m = illumination.shape[-1] // 4
        self.slots = offsets.shape[2]
        self.half = self.n // 2
        assert self.nty == 2 and self.slots == self.n and self.n & (self.n - 1) == 0
        assert self.t == illumination.shape[-1] == self.n * self.h == 4 * self.m

    def window_of(self, device, row, home):
        return device if home else device - row * self.half

    def holds(self, device, row, home):
        return 0 <= self.window_of(device, row, home) < self.half

    def inward(self, s, home):
        n = self.n
        return [(a * n + p, a * n + (p ^ s)) for a in range(2) for p in range(n) if self.holds(p ^ s, a, home)]

    def outward(self, s):
        return [(d, o) for o, d in self.inward(s, False)]


def complete(pairs, n):
    sources, targets = {x for x, _ in pairs}, {y for _, y in pairs}
    other = lambda x: (x + n) % (2 * n)
    extra = [(x, other(x)) for x in range(2 * n) if x not in sources and other(x) not in targets]
    return pairs + extra if len(pairs) + len(extra) == 2 * n else pairs


def where_am_i():
    return lax.axis_index("ty"), lax.axis_index("tx"), lax.axis_index("pos")


def masks(place_ref, k, a, p, lay):
    h, t, m = lay.h, lay.t, lay.m
    k = jnp.clip(k, 0, lay.slots - 1)
    top = place_ref[0, 0, 0, k] - m
    left = place_ref[0, 0, 1, k] - m
    rows = iota((h, t), 0) + p * h
    cols = iota((h, t), 1)
    above = rows >= top + t
    below = rows < top
    outside = above | below
    partner = (above & (a == 1)) | (below & (a == 0))
    halo = (cols >= left + t) | (cols < left)
    return outside, partner, halo


def pack_blocks(place_ref, own, own_halo, prt, prt_halo, out_refs, lay, home):
    a, _, p = where_am_i()
    for s in range(lay.n):
        k = lay.window_of(p ^ s, a, home)
        outside, partner, halo = masks(place_ref, k, a, p, lay)
        for c in range(4):
            mine = jnp.where(halo, spread(own_halo[c], lay), own[c])
            theirs = jnp.where(halo, spread(prt_halo[c], lay), prt[c])
            value = jnp.where(partner, theirs, jnp.where(outside, 0.0, mine))
            if home:
                out_refs[c // 2 * lay.n + s][c % 2] = value
            else:
                out_refs[s][c] = value


def spread(halo, lay):
    return halo if lay.t == 2 * lay.m else jnp.concatenate([halo, halo], axis=1)


def roll_half(x, lay):
    return pltpu.roll(x, lay.m, 1)


def kernel_strips(lay):
    t, m = lay.t, lay.m

    def body(own_ref, prt_ref, out_ref):
        a = lax.axis_index("ty")
        low = iota((lay.h, 2 * m), 1) < m
        for c in range(4):
            for row in (0, 1):

                @pl.when(a == row)
                def _(c=c, row=row):
                    cut = slice(t - 2 * m, t) if row == 0 else slice(0, 2 * m)
                    first, second = (own_ref, prt_ref) if row == 0 else (prt_ref, own_ref)
                    x0, x1 = first[c, :, cut], roll_half(second[c, :, cut], lay)
                    out_ref[c] = jnp.where(low, x1, x0) if row == 0 else jnp.where(low, x0, x1)

    return body


def kernel_pack(lay):
    m = lay.m

    def body(place_ref, own_ref, prt_ref, mine_ref, theirs_ref, *outs):
        a, b, _ = where_am_i()
        blocks, own_halo_ref, prt_halo_ref = outs[: lay.n], outs[lay.n], outs[lay.n + 1]
        low = iota((lay.h, 2 * m), 1) < m
        keep = jnp.where(low, (b < lay.ntx - 1).astype(F32), (b > 0).astype(F32))
        for c in range(4):
            from_left = jnp.where(a == 0, mine_ref[c], theirs_ref[c])
            from_right = jnp.where(a == 0, theirs_ref[c], mine_ref[c])
            halo0 = jnp.where(low, from_right, from_left)
            halo1 = jnp.where(low, roll_half(from_right, lay), roll_half(from_left, lay))
            own_halo_ref[c] = jnp.where(keep > 0, jnp.where(a == 0, halo0, halo1), 0.0)
            prt_halo_ref[c] = jnp.where(keep > 0, jnp.where(a == 0, halo1, halo0), 0.0)
        pack_blocks(place_ref, own_ref, own_halo_ref, prt_ref, prt_halo_ref, blocks, lay, False)

    return body


def move(target, *arrays):
    count = len(arrays)
    inward = target is pltpu.VMEM
    here, there = vmem(), pl.BlockSpec(memory_space=pl.ANY)

    def body(*refs):
        sources, targets, sems = refs[:count], refs[count : 2 * count], refs[2 * count]
        copies = [pltpu.make_async_copy(x, y, sems.at[i]) for i, (x, y) in enumerate(zip(sources, targets))]
        for copy in copies:
            copy.start()
        for copy in copies:
            copy.wait()

    return pl.pallas_call(
        body,
        out_shape=tuple(target(x.shape, x.dtype) for x in arrays),
        in_specs=[there if inward else here] * count,
        out_specs=tuple(here if inward else there for _ in arrays),
        scratch_shapes=[pltpu.SemaphoreType.DMA((count,))],
        compiler_params=pltpu.CompilerParams(vmem_limit_bytes=2 * 1024 * 1024),
    )(*[pltpu.with_memory_space_constraint(x, pltpu.HBM if inward else pltpu.VMEM) for x in arrays])


def kernel_slab(phase_ref, slab_ref):
    slab_ref[0] = jnp.cos(phase_ref[...])
    slab_ref[1] = jnp.sin(phase_ref[...])


def kernel_probe(lay):
    def body(place_ref, light_ref, out_ref):
        a, _, p = where_am_i()
        for i, home in enumerate((False, True)):
            k = jnp.clip(lay.window_of(p, a, home), 0, lay.slots - 1)
            down = (place_ref[0, 0, 0, k] + (lay.t - lay.m)) % lay.t
            along = (place_ref[0, 0, 1, k] + (lay.t - lay.m)) % lay.t
            for c in range(2):
                out_ref[i, c] = pltpu.roll(pltpu.roll(light_ref[c], down, 0), along, 1)

    return body


def assemble(blocks, window_ref, lay):
    p = lax.axis_index("pos")
    for s in range(lay.n):
        start = pl.multiple_of((p ^ s) * lay.h, lay.h)
        for c in range(window_ref.shape[0]):
            window_ref[c, pl.ds(start, lay.h), :] = blocks[s][c]


def propagate(o1r, o1i, light_ref, which, slab_ref, tab):
    er, ei = cmul(light_ref[which, 0], light_ref[which, 1], o1r, o1i)
    sr, si = transform(er, ei, tab, False)
    sr, si = cmul(sr, si, slab_ref[0], slab_ref[1])
    return transform(sr, si, tab, True)


def kernel_gradient(lay):
    def body(count_ref, *refs):
        n = lay.n
        blocks, (light_ref, slab_ref, tab, meas_ref, moved_ref) = refs[:n], refs[n : n + 5]
        outs, window_ref = refs[n + 5 : 2 * n + 5], refs[2 * n + 5]
        a, _, p = where_am_i()
        k = lay.window_of(p, a, False)

        @pl.when((k >= 0) & (k < count_ref[0, 0]))
        def _():
            assemble(blocks, window_ref, lay)
            br, bi = propagate(window_ref[0], window_ref[1], light_ref, 0, slab_ref, tab)
            lr, li = cmul(br, bi, window_ref[2], window_ref[3])
            fr, fi = transform(lr, li, tab, False)
            seen = jnp.where(a == 0, meas_ref[0, 0, 0], moved_ref[0, 0, 0])
            keeping = 1.0 - seen / jnp.maximum(jnp.sqrt(fr * fr + fi * fi), magnitude_floor)
            kr, ki = transform(fr * keeping, fi * keeping, tab, True)
            g2r, g2i = cmul(br, -bi, kr, ki)
            tr, ti = cmul(window_ref[2], -window_ref[3], kr, ki)
            window_ref[2] = g2r
            window_ref[3] = g2i
            sr, si = transform(tr, ti, tab, False)
            sr, si = cmul(sr, si, slab_ref[0], -slab_ref[1])
            ir, ii = transform(sr, si, tab, True)
            g1r, g1i = cmul(light_ref[0, 0], -light_ref[0, 1], ir, ii)
            window_ref[0] = g1r
            window_ref[1] = g1i
            for s in range(n):
                start = pl.multiple_of((p ^ s) * lay.h, lay.h)
                for c in range(4):
                    outs[s][c] = window_ref[c, pl.ds(start, lay.h), :]

    return body


def kernel_collect(lay):
    t, m = lay.t, lay.m

    def body(place_ref, count_ref, *refs):
        n = lay.n
        blocks, mom_ref = refs[:n], refs[n]
        own_ref, halo_ref = refs[n + 1 :]
        a, _, p = where_am_i()
        low = iota((lay.h, 2 * m), 1) < m
        own_ref[0] = momentum_rate * mom_ref[...]
        own_ref[1] = jnp.zeros(own_ref.shape[1:], F32)
        halo_ref[...] = jnp.zeros(halo_ref.shape, F32)
        for s in range(n):
            k = lay.window_of(p ^ s, a, False)

            @pl.when((k >= 0) & (k < count_ref[0, 0]))
            def _(s=s, k=k):
                outside, partner, halo = masks(place_ref, k, a, p, lay)
                for c in range(4):
                    g = blocks[s][c]
                    for i, rows in enumerate((~outside, partner)):
                        own_ref[i, c] += jnp.where(rows & ~halo, g, 0.0)
                        x = jnp.where(rows & halo, g, 0.0)
                        halo_ref[i, c] += jnp.where(low, x[:, : 2 * m], x[:, t - 2 * m :])

    return body


def kernel_strips_back(lay):
    t, m = lay.t, lay.m

    def body(own_ref, halo_ref, their_own_ref, their_halo_ref, sum_ref, halo_sum_ref, out_ref):
        a = lax.axis_index("ty")
        low = iota((lay.h, 2 * m), 1) < m
        for c in range(4):
            for i in range(2):
                sum_ref[i, c] = own_ref[i, c] + their_own_ref[1 - i, c]
                halo_sum_ref[i, c] = halo_ref[i, c] + their_halo_ref[1 - i, c]
        for row in (0, 1):

            @pl.when(a == row)
            def _(row=row):
                for tile in range(2):
                    i = tile ^ row
                    for c in range(4):
                        halo = halo_sum_ref[i, c]
                        if row == 0:
                            out_ref[tile, c] = jnp.where(low, halo, sum_ref[i, c, :, t - 2 * m :])
                        else:
                            out_ref[tile, c] = jnp.where(low, sum_ref[i, c, :, : 2 * m], halo)

    return body


def kernel_update(lay):
    m = lay.m

    def body(place_ref, obj_ref, prt_ref, obj_halo_ref, prt_halo_ref, sum_ref, halo_sum_ref, mine_ref, theirs_ref, *outs):
        n = lay.n
        new_ref, vel_ref, *blocks = outs[: 2 * n + 2]
        prt_new, own_halo, prt_halo = outs[2 * n + 2 :]
        a, b, _ = where_am_i()
        low = iota((lay.h, 2 * m), 1) < m
        not_first, not_last = b > 0, b < lay.ntx - 1
        keep = (low & not_last) | (~low & not_first)
        for i in range(2):
            tile = a if i == 0 else 1 - a
            for c in range(4):
                mine, theirs = mine_ref[tile, c], theirs_ref[tile, c]
                from_left = jnp.where(not_first, jnp.where(a == 0, mine, theirs), 0.0)
                from_right = jnp.where(not_last, jnp.where(a == 0, theirs, mine), 0.0)
                v = sum_ref[i, c] + jnp.concatenate(
                    [jnp.where(low, from_left, 0.0), jnp.where(low, 0.0, from_right)], axis=1
                )
                hv = halo_sum_ref[i, c] + jnp.where(low, from_right, from_left)
                obj, halo = (obj_ref, obj_halo_ref) if i == 0 else (prt_ref, prt_halo_ref)
                new, new_halo = (new_ref, own_halo) if i == 0 else (prt_new, prt_halo)
                if i == 0:
                    vel_ref[c] = v
                new[c] = obj[c] - step_length * v
                new_halo[c] = jnp.where(keep, halo[c] - step_length * hv, 0.0)
        pack_blocks(place_ref, new_ref, own_halo, prt_new, prt_halo, blocks, lay, True)

    return body


def kernel_between(lay):
    def body(count_ref, *refs):
        n = lay.n
        blocks, (light_ref, slab_ref, tab), out_ref, window_ref = refs[:n], refs[n : n + 3], refs[n + 3], refs[n + 4]

        @pl.when(lax.axis_index("pos") < count_ref[0, 0])
        def _():
            assemble(blocks, window_ref, lay)
            out_ref[0], out_ref[1] = propagate(window_ref[0], window_ref[1], light_ref, 1, slab_ref, tab)

    return body


def kernel_predict(lay):
    def body(count_ref, *refs):
        n = lay.n
        blocks, (between_ref, tab), out_ref, window_ref = refs[:n], refs[n : n + 2], refs[n + 2], refs[n + 3]
        live = lax.axis_index("pos") < count_ref[0, 0]

        @pl.when(live)
        def _():
            assemble(blocks, window_ref, lay)
            lr, li = cmul(between_ref[0], between_ref[1], window_ref[0], window_ref[1])
            fr, fi = transform(lr, li, tab, False)
            out_ref[0, 0, 0] = jnp.sqrt(fr * fr + fi * fi)

        @pl.when(jnp.logical_not(live))
        def _():
            out_ref[...] = jnp.zeros(out_ref.shape, F32)

    return body


def iteration(object_field, momentum, measured, illumination, slab_phase, offsets, entry_counts):
    lay = Layout(object_field, illumination, offsets)
    n, h, t, m = lay.n, lay.h, lay.t, lay.m
    own = object_field.reshape(4, h, t)
    offsets = offsets.transpose(0, 1, 3, 2)
    velocity_old = momentum.reshape(4, h, t)
    block, halo_shape = (4, h, t), (4, h, 2 * m)
    tab = jnp.asarray(dft_tables(t))
    cores = lambda x: lax.ppermute(x, "ty", [(0, 1), (1, 0)])
    partner = cores(own)
    own, velocity_old, measured, illumination, slab_phase, tab = move(
        pltpu.VMEM, own, velocity_old, measured, illumination, slab_phase, tab
    )
    ntx = lay.ntx
    shift = [(b, b + 1) for b in range(ntx - 1)] + [(ntx - 1, 2 * ntx - 1)]
    shift += [(ntx + b + 1, ntx + b) for b in range(ntx - 1)] + [(ntx, 0)]
    columns = lambda x: lax.ppermute(x, ("ty", "tx"), shift)

    def exchange(values, pairs_of):
        got = [values[0]]
        for s in range(1, n):
            got.append(lax.ppermute(values[s], ("ty", "pos"), complete(pairs_of(s), n)))
        return got

    moved = lax.ppermute(measured, "pos", [(p, p ^ lay.half) for p in range(n)])
    (slab,) = call(kernel_slab, [(2, t, t)], [slab_phase])
    (light,) = call(kernel_probe(lay), [(2, 2, t, t)], [offsets, illumination], 1)

    (strips,) = call(kernel_strips(lay), [halo_shape], [own, partner])
    strips = columns(strips)
    strips_other = cores(strips)
    *blocks, own_halo, partner_halo = call(
        kernel_pack(lay), [block] * n + [halo_shape] * 2, [offsets, own, partner, strips, strips_other], 1
    )
    received = exchange(blocks, lambda s: lay.inward(s, False))
    window = pltpu.VMEM((4, t, t), F32)
    terms = call(
        kernel_gradient(lay),
        [block] * n,
        [entry_counts, *received, light, slab, tab, measured, moved],
        1,
        [window],
        limit=24,
    )
    parts = exchange(terms, lay.outward)
    sums, halos = call(
        kernel_collect(lay), [(2, *block), (2, *halo_shape)], [offsets, entry_counts, *parts, velocity_old], 2
    )
    sums, halos, strips = call(
        kernel_strips_back(lay),
        [(2, *block), (2, *halo_shape), (2, *halo_shape)],
        [sums, halos, cores(sums), cores(halos)],
    )
    strips = columns(strips)
    updated, velocity, *rest = call(
        kernel_update(lay),
        [block] * 2 + [(2, h, t)] * (2 * n),
        [offsets, own, partner, own_halo, partner_halo, sums, halos, strips, cores(strips)],
        1,
        [pltpu.VMEM(block, F32), pltpu.VMEM(halo_shape, F32), pltpu.VMEM(halo_shape, F32)],
    )
    first = exchange(rest[:n], lambda s: lay.inward(s, True))
    second = exchange(rest[n : 2 * n], lambda s: lay.inward(s, True))
    updated, velocity = move(pltpu.HBM, updated, velocity)
    half_window = pltpu.VMEM((2, t, t), F32)
    (between,) = call(
        kernel_between(lay), [(2, t, t)], [entry_counts, *first, light, slab, tab], 1, [half_window], limit=24
    )
    (amplitudes,) = call(
        kernel_predict(lay),
        [measured.shape],
        [entry_counts, *second, between, tab],
        1,
        [half_window],
        limit=24,
        last=True,
    )
    return (
        updated.reshape(object_field.shape),
        velocity.reshape(momentum.shape),
        amplitudes,
    )


def solution(mesh):
    placed = (
        P(None, None, ("ty", "pos"), "tx"),
        P(None, None, ("ty", "pos"), "tx"),
        P("ty", "tx", "pos", None, None),
        P(),
        P(),
        P("ty", "tx", None, None),
        P("ty", "tx"),
    )
    return jax.shard_map(
        iteration,
        mesh=mesh,
        in_specs=placed,
        out_specs=(
            P(None, None, ("ty", "pos"), "tx"),
            P(None, None, ("ty", "pos"), "tx"),
            P("ty", "tx", "pos", None, None),
        ),
        check_vma=False,
    )
```

```python
import math

import jax
import jax.numpy as jnp
import numpy as np
from jax import lax
from jax.experimental import pallas as pl
from jax.experimental.pallas import tpu as pltpu
from jax.sharding import PartitionSpec as P


magnitude_floor = 0.5
momentum_rate = 0.9
step_length = 0.05
F32 = jnp.float32
BF16 = jnp.bfloat16


def vmem():
    return pl.BlockSpec(memory_space=pltpu.VMEM)


def smem():
    return pl.BlockSpec(memory_space=pltpu.SMEM)


def call(body, outs, args, scalars=0, scratch=(), limit=8, last=False):
    specs = [smem()] * scalars + [vmem()] * (len(args) - scalars)
    placed = [pltpu.with_memory_space_constraint(x, pltpu.VMEM) for x in args[scalars:]]
    return pl.pallas_call(
        body,
        out_shape=tuple((jax.ShapeDtypeStruct if last else pltpu.VMEM)(s, F32) for s in outs),
        in_specs=specs,
        out_specs=tuple(vmem() for _ in outs),
        scratch_shapes=list(scratch),
        compiler_params=pltpu.CompilerParams(vmem_limit_bytes=limit * 1024 * 1024),
    )(*args[:scalars], *placed)


def split_table(values):
    high = values.astype(jnp.bfloat16)
    low = (values - high.astype(np.float64)).astype(jnp.bfloat16)
    return high, low


def dft_tables(length):
    index = np.arange(length)
    angles = (index[:, None] * index[None, :] % length) * (2.0 * math.pi / length)
    cosine, sine = np.cos(angles) / math.sqrt(length), np.sin(angles) / math.sqrt(length)
    parts = [part for t in (cosine, cosine + sine, cosine - sine) for part in split_table(t)]
    return np.stack(parts)


def iota(shape, dim):
    return lax.broadcasted_iota(jnp.int32, shape, dim)


def split(value):
    high = value.astype(BF16)
    return high, (value - high.astype(F32)).astype(BF16)


def dot(left, right):
    return jnp.dot(left, right, preferred_element_type=F32)


def mul3(left, right):
    return dot(left[0], right[0]) + dot(left[0], right[1]) + dot(left[1], right[0])


def transform(real, imag, tab, inverse):
    cos = (tab[0], tab[1])
    plus, minus = ((tab[4], tab[5]), (tab[2], tab[3])) if inverse else ((tab[2], tab[3]), (tab[4], tab[5]))
    both = mul3(split(real + imag), cos)
    right_imag = both - mul3(split(real), plus)
    left_low = mul3(minus, split(right_imag))
    right_real = both - mul3(split(imag), minus)
    both = mul3(cos, split(right_real + right_imag))
    return both - left_low, both - mul3(plus, split(right_real))


def cmul(ar, ai, br, bi):
    return ar * br - ai * bi, ar * bi + ai * br


class Layout:
    def __init__(self, object_field, illumination, offsets):
        self.n = lax.axis_size("pos")
        self.ntx = lax.axis_size("tx")
        self.nty = lax.axis_size("ty")
        self.h = object_field.shape[2]
        self.t = object_field.shape[3]
        self.m = illumination.shape[-1] // 4
        self.slots = offsets.shape[2]
        self.half = self.n // 2
        assert self.nty == 2 and self.slots == self.n and self.n & (self.n - 1) == 0
        assert self.t == illumination.shape[-1] == self.n * self.h == 4 * self.m

    def window_of(self, device, row, home):
        return device if home else device - row * self.half

    def holds(self, device, row, home):
        return 0 <= self.window_of(device, row, home) < self.half

    def inward(self, s, home):
        n = self.n
        return [(a * n + p, a * n + (p ^ s)) for a in range(2) for p in range(n) if self.holds(p ^ s, a, home)]

    def outward(self, s):
        return [(d, o) for o, d in self.inward(s, False)]


def complete(pairs, n):
    sources, targets = {x for x, _ in pairs}, {y for _, y in pairs}
    other = lambda x: (x + n) % (2 * n)
    extra = [(x, other(x)) for x in range(2 * n) if x not in sources and other(x) not in targets]
    return pairs + extra if len(pairs) + len(extra) == 2 * n else pairs


def where_am_i():
    return lax.axis_index("ty"), lax.axis_index("tx"), lax.axis_index("pos")


def masks(place_ref, k, a, p, lay):
    h, t, m = lay.h, lay.t, lay.m
    k = jnp.clip(k, 0, lay.slots - 1)
    top = place_ref[0, 0, 0, k] - m
    left = place_ref[0, 0, 1, k] - m
    rows = iota((h, t), 0) + p * h
    cols = iota((h, t), 1)
    above = rows >= top + t
    below = rows < top
    outside = above | below
    partner = (above & (a == 1)) | (below & (a == 0))
    halo = (cols >= left + t) | (cols < left)
    return outside, partner, halo


def pack_blocks(place_ref, own, own_halo, prt, prt_halo, out_refs, lay, home):
    a, _, p = where_am_i()
    for s in range(lay.n):
        k = lay.window_of(p ^ s, a, home)
        outside, partner, halo = masks(place_ref, k, a, p, lay)
        for c in range(4):
            mine = jnp.where(halo, spread(own_halo[c], lay), own[c])
            theirs = jnp.where(halo, spread(prt_halo[c], lay), prt[c])
            value = jnp.where(partner, theirs, jnp.where(outside, 0.0, mine))
            if home:
                out_refs[c // 2 * lay.n + s][c % 2] = value
            else:
                out_refs[s][c] = value


def spread(halo, lay):
    return halo if lay.t == 2 * lay.m else jnp.concatenate([halo, halo], axis=1)


def roll_half(x, lay):
    return pltpu.roll(x, lay.m, 1)


def kernel_strips(lay):
    t, m = lay.t, lay.m

    def body(own_ref, prt_ref, out_ref):
        a = lax.axis_index("ty")
        low = iota((lay.h, 2 * m), 1) < m
        for c in range(4):
            for row in (0, 1):

                @pl.when(a == row)
                def _(c=c, row=row):
                    cut = slice(t - 2 * m, t) if row == 0 else slice(0, 2 * m)
                    first, second = (own_ref, prt_ref) if row == 0 else (prt_ref, own_ref)
                    x0, x1 = first[c, :, cut], roll_half(second[c, :, cut], lay)
                    out_ref[c] = jnp.where(low, x1, x0) if row == 0 else jnp.where(low, x0, x1)

    return body


def kernel_pack(lay):
    m = lay.m

    def body(place_ref, own_ref, prt_ref, mine_ref, theirs_ref, *outs):
        a, b, _ = where_am_i()
        blocks, own_halo_ref, prt_halo_ref = outs[: lay.n], outs[lay.n], outs[lay.n + 1]
        low = iota((lay.h, 2 * m), 1) < m
        keep = jnp.where(low, (b < lay.ntx - 1).astype(F32), (b > 0).astype(F32))
        for c in range(4):
            from_left = jnp.where(a == 0, mine_ref[c], theirs_ref[c])
            from_right = jnp.where(a == 0, theirs_ref[c], mine_ref[c])
            halo0 = jnp.where(low, from_right, from_left)
            halo1 = jnp.where(low, roll_half(from_right, lay), roll_half(from_left, lay))
            own_halo_ref[c] = jnp.where(keep > 0, jnp.where(a == 0, halo0, halo1), 0.0)
            prt_halo_ref[c] = jnp.where(keep > 0, jnp.where(a == 0, halo1, halo0), 0.0)
        pack_blocks(place_ref, own_ref, own_halo_ref, prt_ref, prt_halo_ref, blocks, lay, False)

    return body


def move(target, *arrays):
    count = len(arrays)
    inward = target is pltpu.VMEM
    here, there = vmem(), pl.BlockSpec(memory_space=pl.ANY)

    def body(*refs):
        sources, targets, sems = refs[:count], refs[count : 2 * count], refs[2 * count]
        copies = [pltpu.make_async_copy(x, y, sems.at[i]) for i, (x, y) in enumerate(zip(sources, targets))]
        for copy in copies:
            copy.start()
        for copy in copies:
            copy.wait()

    return pl.pallas_call(
        body,
        out_shape=tuple(target(x.shape, x.dtype) for x in arrays),
        in_specs=[there if inward else here] * count,
        out_specs=tuple(here if inward else there for _ in arrays),
        scratch_shapes=[pltpu.SemaphoreType.DMA((count,))],
        compiler_params=pltpu.CompilerParams(vmem_limit_bytes=2 * 1024 * 1024),
    )(*[pltpu.with_memory_space_constraint(x, pltpu.HBM if inward else pltpu.VMEM) for x in arrays])


def kernel_slab(phase_ref, slab_ref):
    slab_ref[0] = jnp.cos(phase_ref[...])
    slab_ref[1] = jnp.sin(phase_ref[...])


def kernel_probe(lay):
    def body(place_ref, light_ref, out_ref):
        a, _, p = where_am_i()
        for i, home in enumerate((False, True)):
            k = jnp.clip(lay.window_of(p, a, home), 0, lay.slots - 1)
            down = (place_ref[0, 0, 0, k] + (lay.t - lay.m)) % lay.t
            along = (place_ref[0, 0, 1, k] + (lay.t - lay.m)) % lay.t
            for c in range(2):
                out_ref[i, c] = pltpu.roll(pltpu.roll(light_ref[c], down, 0), along, 1)

    return body


def assemble(blocks, window_ref, lay):
    p = lax.axis_index("pos")
    for s in range(lay.n):
        start = pl.multiple_of((p ^ s) * lay.h, lay.h)
        for c in range(window_ref.shape[0]):
            window_ref[c, pl.ds(start, lay.h), :] = blocks[s][c]


def propagate(o1r, o1i, light_ref, which, slab_ref, tab):
    er, ei = cmul(light_ref[which, 0], light_ref[which, 1], o1r, o1i)
    sr, si = transform(er, ei, tab, False)
    sr, si = cmul(sr, si, slab_ref[0], slab_ref[1])
    return transform(sr, si, tab, True)


def kernel_gradient(lay):
    def body(count_ref, *refs):
        n = lay.n
        blocks, (light_ref, slab_ref, tab, meas_ref, moved_ref) = refs[:n], refs[n : n + 5]
        outs, window_ref = refs[n + 5 : 2 * n + 5], refs[2 * n + 5]
        a, _, p = where_am_i()
        k = lay.window_of(p, a, False)

        @pl.when((k >= 0) & (k < count_ref[0, 0]))
        def _():
            assemble(blocks, window_ref, lay)
            br, bi = propagate(window_ref[0], window_ref[1], light_ref, 0, slab_ref, tab)
            lr, li = cmul(br, bi, window_ref[2], window_ref[3])
            fr, fi = transform(lr, li, tab, False)
            seen = jnp.where(a == 0, meas_ref[0, 0, 0], moved_ref[0, 0, 0])
            keeping = 1.0 - seen / jnp.maximum(jnp.sqrt(fr * fr + fi * fi), magnitude_floor)
            kr, ki = transform(fr * keeping, fi * keeping, tab, True)
            g2r, g2i = cmul(br, -bi, kr, ki)
            tr, ti = cmul(window_ref[2], -window_ref[3], kr, ki)
            window_ref[2] = g2r
            window_ref[3] = g2i
            sr, si = transform(tr, ti, tab, False)
            sr, si = cmul(sr, si, slab_ref[0], -slab_ref[1])
            ir, ii = transform(sr, si, tab, True)
            g1r, g1i = cmul(light_ref[0, 0], -light_ref[0, 1], ir, ii)
            window_ref[0] = g1r
            window_ref[1] = g1i
            for s in range(n):
                start = pl.multiple_of((p ^ s) * lay.h, lay.h)
                for c in range(4):
                    outs[s][c] = window_ref[c, pl.ds(start, lay.h), :]

    return body


def kernel_collect(lay):
    t, m = lay.t, lay.m

    def body(place_ref, count_ref, *refs):
        n = lay.n
        blocks, mom_ref = refs[:n], refs[n]
        own_ref, halo_ref = refs[n + 1 :]
        a, _, p = where_am_i()
        low = iota((lay.h, 2 * m), 1) < m
        own_ref[0] = momentum_rate * mom_ref[...]
        own_ref[1] = jnp.zeros(own_ref.shape[1:], F32)
        halo_ref[...] = jnp.zeros(halo_ref.shape, F32)
        for s in range(n):
            k = lay.window_of(p ^ s, a, False)

            @pl.when((k >= 0) & (k < count_ref[0, 0]))
            def _(s=s, k=k):
                outside, partner, halo = masks(place_ref, k, a, p, lay)
                for c in range(4):
                    g = blocks[s][c]
                    for i, rows in enumerate((~outside, partner)):
                        own_ref[i, c] += jnp.where(rows & ~halo, g, 0.0)
                        x = jnp.where(rows & halo, g, 0.0)
                        halo_ref[i, c] += jnp.where(low, x[:, : 2 * m], x[:, t - 2 * m :])

    return body


def kernel_strips_back(lay):
    t, m = lay.t, lay.m

    def body(own_ref, halo_ref, their_own_ref, their_halo_ref, sum_ref, halo_sum_ref, out_ref):
        a = lax.axis_index("ty")
        low = iota((lay.h, 2 * m), 1) < m
        for c in range(4):
            for i in range(2):
                sum_ref[i, c] = own_ref[i, c] + their_own_ref[1 - i, c]
                halo_sum_ref[i, c] = halo_ref[i, c] + their_halo_ref[1 - i, c]
        for row in (0, 1):

            @pl.when(a == row)
            def _(row=row):
                for tile in range(2):
                    i = tile ^ row
                    for c in range(4):
                        halo = halo_sum_ref[i, c]
                        if row == 0:
                            out_ref[tile, c] = jnp.where(low, halo, sum_ref[i, c, :, t - 2 * m :])
                        else:
                            out_ref[tile, c] = jnp.where(low, sum_ref[i, c, :, : 2 * m], halo)

    return body


def kernel_update(lay):
    m = lay.m

    def body(place_ref, obj_ref, prt_ref, obj_halo_ref, prt_halo_ref, sum_ref, halo_sum_ref, mine_ref, theirs_ref, *outs):
        n = lay.n
        new_ref, vel_ref, *blocks = outs[: 2 * n + 2]
        prt_new, own_halo, prt_halo = outs[2 * n + 2 :]
        a, b, _ = where_am_i()
        low = iota((lay.h, 2 * m), 1) < m
        not_first, not_last = b > 0, b < lay.ntx - 1
        keep = (low & not_last) | (~low & not_first)
        for i in range(2):
            tile = a if i == 0 else 1 - a
            for c in range(4):
                mine, theirs = mine_ref[tile, c], theirs_ref[tile, c]
                from_left = jnp.where(not_first, jnp.where(a == 0, mine, theirs), 0.0)
                from_right = jnp.where(not_last, jnp.where(a == 0, theirs, mine), 0.0)
                v = sum_ref[i, c] + jnp.concatenate(
                    [jnp.where(low, from_left, 0.0), jnp.where(low, 0.0, from_right)], axis=1
                )
                hv = halo_sum_ref[i, c] + jnp.where(low, from_right, from_left)
                obj, halo = (obj_ref, obj_halo_ref) if i == 0 else (prt_ref, prt_halo_ref)
                new, new_halo = (new_ref, own_halo) if i == 0 else (prt_new, prt_halo)
                if i == 0:
                    vel_ref[c] = v
                new[c] = obj[c] - step_length * v
                new_halo[c] = jnp.where(keep, halo[c] - step_length * hv, 0.0)
        pack_blocks(place_ref, new_ref, own_halo, prt_new, prt_halo, blocks, lay, True)

    return body


def kernel_between(lay):
    def body(count_ref, *refs):
        n = lay.n
        blocks, (light_ref, slab_ref, tab), out_ref, window_ref = refs[:n], refs[n : n + 3], refs[n + 3], refs[n + 4]

        @pl.when(lax.axis_index("pos") < count_ref[0, 0])
        def _():
            assemble(blocks, window_ref, lay)
            out_ref[0], out_ref[1] = propagate(window_ref[0], window_ref[1], light_ref, 1, slab_ref, tab)

    return body


def kernel_predict(lay):
    def body(count_ref, *refs):
        n = lay.n
        blocks, (between_ref, tab), out_ref, window_ref = refs[:n], refs[n : n + 2], refs[n + 2], refs[n + 3]
        live = lax.axis_index("pos") < count_ref[0, 0]

        @pl.when(live)
        def _():
            assemble(blocks, window_ref, lay)
            lr, li = cmul(between_ref[0], between_ref[1], window_ref[0], window_ref[1])
            fr, fi = transform(lr, li, tab, False)
            out_ref[0, 0, 0] = jnp.sqrt(fr * fr + fi * fi)

        @pl.when(jnp.logical_not(live))
        def _():
            out_ref[...] = jnp.zeros(out_ref.shape, F32)

    return body


def iteration(object_field, momentum, measured, illumination, slab_phase, offsets, entry_counts):
    lay = Layout(object_field, illumination, offsets)
    n, h, t, m = lay.n, lay.h, lay.t, lay.m
    own = object_field.reshape(4, h, t)
    offsets = offsets.transpose(0, 1, 3, 2)
    velocity_old = momentum.reshape(4, h, t)
    block, halo_shape = (4, h, t), (4, h, 2 * m)
    tab = jnp.asarray(dft_tables(t))
    cores = lambda x: lax.ppermute(x, "ty", [(0, 1), (1, 0)])
    partner = cores(own)
    own, velocity_old, measured, illumination, slab_phase, tab = move(
        pltpu.VMEM, own, velocity_old, measured, illumination, slab_phase, tab
    )
    ntx = lay.ntx
    shift = [(b, b + 1) for b in range(ntx - 1)] + [(ntx - 1, 2 * ntx - 1)]
    shift += [(ntx + b + 1, ntx + b) for b in range(ntx - 1)] + [(ntx, 0)]
    columns = lambda x: lax.ppermute(x, ("ty", "tx"), shift)

    def exchange(values, pairs_of):
        got = [values[0]]
        for s in range(1, n):
            got.append(lax.ppermute(values[s], ("ty", "pos"), complete(pairs_of(s), n)))
        return got

    moved = lax.ppermute(measured, "pos", [(p, p ^ lay.half) for p in range(n)])
    (slab,) = call(kernel_slab, [(2, t, t)], [slab_phase])
    (light,) = call(kernel_probe(lay), [(2, 2, t, t)], [offsets, illumination], 1)

    (strips,) = call(kernel_strips(lay), [halo_shape], [own, partner])
    strips = columns(strips)
    strips_other = cores(strips)
    *blocks, own_halo, partner_halo = call(
        kernel_pack(lay), [block] * n + [halo_shape] * 2, [offsets, own, partner, strips, strips_other], 1
    )
    received = exchange(blocks, lambda s: lay.inward(s, False))
    window = pltpu.VMEM((4, t, t), F32)
    terms = call(
        kernel_gradient(lay),
        [block] * n,
        [entry_counts, *received, light, slab, tab, measured, moved],
        1,
        [window],
        limit=24,
    )
    parts = exchange(terms, lay.outward)
    sums, halos = call(
        kernel_collect(lay), [(2, *block), (2, *halo_shape)], [offsets, entry_counts, *parts, velocity_old], 2
    )
    sums, halos, strips = call(
        kernel_strips_back(lay),
        [(2, *block), (2, *halo_shape), (2, *halo_shape)],
        [sums, halos, cores(sums), cores(halos)],
    )
    strips = columns(strips)
    updated, velocity, *rest = call(
        kernel_update(lay),
        [block] * 2 + [(2, h, t)] * (2 * n),
        [offsets, own, partner, own_halo, partner_halo, sums, halos, strips, cores(strips)],
        1,
        [pltpu.VMEM(block, F32), pltpu.VMEM(halo_shape, F32), pltpu.VMEM(halo_shape, F32)],
    )
    first = exchange(rest[:n], lambda s: lay.inward(s, True))
    second = exchange(rest[n : 2 * n], lambda s: lay.inward(s, True))
    updated, velocity = move(pltpu.HBM, updated, velocity)
    half_window = pltpu.VMEM((2, t, t), F32)
    (between,) = call(
        kernel_between(lay), [(2, t, t)], [entry_counts, *first, light, slab, tab], 1, [half_window], limit=24
    )
    (amplitudes,) = call(
        kernel_predict(lay),
        [measured.shape],
        [entry_counts, *second, between, tab],
        1,
        [half_window],
        limit=24,
        last=True,
    )
    return (
        updated.reshape(object_field.shape),
        velocity.reshape(momentum.shape),
        amplitudes,
    )


def solution(mesh):
    placed = (
        P(None, None, ("ty", "pos"), "tx"),
        P(None, None, ("ty", "pos"), "tx"),
        P("ty", "tx", "pos", None, None),
        P(),
        P(),
        P("ty", "tx", None, None),
        P("ty", "tx"),
    )
    return jax.shard_map(
        iteration,
        mesh=mesh,
        in_specs=placed,
        out_specs=(
            P(None, None, ("ty", "pos"), "tx"),
            P(None, None, ("ty", "pos"), "tx"),
            P("ty", "tx", "pos", None, None),
        ),
        check_vma=False,
    )
```

```python
import math

import jax
import jax.numpy as jnp
import numpy as np
from jax import lax
from jax.experimental import pallas as pl
from jax.experimental.pallas import tpu as pltpu
from jax.sharding import PartitionSpec as P


magnitude_floor = 0.5
momentum_rate = 0.9
step_length = 0.05
F32 = jnp.float32
BF16 = jnp.bfloat16


def vmem():
    return pl.BlockSpec(memory_space=pltpu.VMEM)


def smem():
    return pl.BlockSpec(memory_space=pltpu.SMEM)


def call(body, outs, args, scalars=0, scratch=(), limit=8, last=False):
    specs = [smem()] * scalars + [vmem()] * (len(args) - scalars)
    placed = [pltpu.with_memory_space_constraint(x, pltpu.VMEM) for x in args[scalars:]]
    return pl.pallas_call(
        body,
        out_shape=tuple((jax.ShapeDtypeStruct if last else pltpu.VMEM)(s, F32) for s in outs),
        in_specs=specs,
        out_specs=tuple(vmem() for _ in outs),
        scratch_shapes=list(scratch),
        compiler_params=pltpu.CompilerParams(vmem_limit_bytes=limit * 1024 * 1024),
    )(*args[:scalars], *placed)


def split_table(values):
    high = values.astype(jnp.bfloat16)
    low = (values - high.astype(np.float64)).astype(jnp.bfloat16)
    return high, low


def dft_tables(length):
    index = np.arange(length)
    angles = (index[:, None] * index[None, :] % length) * (2.0 * math.pi / length)
    cosine, sine = np.cos(angles) / math.sqrt(length), np.sin(angles) / math.sqrt(length)
    parts = [part for t in (cosine, cosine + sine, cosine - sine) for part in split_table(t)]
    return np.stack(parts)


def iota(shape, dim):
    return lax.broadcasted_iota(jnp.int32, shape, dim)


def split(value):
    high = value.astype(BF16)
    return high, (value - high.astype(F32)).astype(BF16)


def dot(left, right):
    return jnp.dot(left, right, preferred_element_type=F32)


def mul3(left, right):
    return dot(left[0], right[0]) + dot(left[0], right[1]) + dot(left[1], right[0])


def transform(real, imag, tab, inverse):
    cos = (tab[0], tab[1])
    plus, minus = ((tab[4], tab[5]), (tab[2], tab[3])) if inverse else ((tab[2], tab[3]), (tab[4], tab[5]))
    both = mul3(split(real + imag), cos)
    right_imag = both - mul3(split(real), plus)
    left_low = mul3(minus, split(right_imag))
    right_real = both - mul3(split(imag), minus)
    both = mul3(cos, split(right_real + right_imag))
    return both - left_low, both - mul3(plus, split(right_real))


def cmul(ar, ai, br, bi):
    return ar * br - ai * bi, ar * bi + ai * br


class Layout:
    def __init__(self, object_field, illumination, offsets):
        self.n = lax.axis_size("pos")
        self.ntx = lax.axis_size("tx")
        self.nty = lax.axis_size("ty")
        self.h = object_field.shape[2]
        self.t = object_field.shape[3]
        self.m = illumination.shape[-1] // 4
        self.slots = offsets.shape[2]
        self.half = self.n // 2
        assert self.nty == 2 and self.slots == self.n and self.n & (self.n - 1) == 0
        assert self.t == illumination.shape[-1] == self.n * self.h == 4 * self.m

    def window_of(self, device, row, home):
        return device if home else device - row * self.half

    def holds(self, device, row, home):
        return 0 <= self.window_of(device, row, home) < self.half

    def crosses(self, s, home):
        return not home and 0 < s < self.half

    def inward(self, s, home):
        n = self.n
        core = (lambda a: 1 - a) if self.crosses(s, home) else (lambda a: a)
        return [(core(a) * n + p, a * n + (p ^ s)) for a in range(2) for p in range(n) if self.holds(p ^ s, a, home)]

    def outward(self, s):
        return [(d, o) for o, d in self.inward(s, False)]


def complete(pairs, n):
    sources, targets = {x for x, _ in pairs}, {y for _, y in pairs}
    other = lambda x: (x + n) % (2 * n)
    extra = [(x, other(x)) for x in range(2 * n) if x not in sources and other(x) not in targets]
    return pairs + extra if len(pairs) + len(extra) == 2 * n else pairs


def where_am_i():
    return lax.axis_index("ty"), lax.axis_index("tx"), lax.axis_index("pos")


def step(lay):
    return min(lay.h, 8)


def by_rows(lay, body):
    for start in range(0, lay.h, step(lay)):
        body(start, slice(start, start + step(lay)))


def masks(place_refs, a, k, p, lay, start):
    h, t, m = lay.h, lay.t, lay.m
    k = jnp.clip(k, 0, lay.slots - 1)
    mine = a == lax.axis_index("ty")
    top, left = (jnp.where(mine, place_refs[0][0, 0, i, k], place_refs[1][0, 0, i, k]) - m for i in range(2))
    rows = iota((step(lay), t), 0) + (p * h + start)
    cols = iota((step(lay), t), 1)
    above = rows >= top + t
    below = rows < top
    outside = above | below
    partner = (above & (a == 1)) | (below & (a == 0))
    halo = (cols >= left + t) | (cols < left)
    return outside, partner, halo


def pack_blocks(place_refs, own, own_halo, prt, prt_halo, out_refs, lay, home):
    a, _, p = where_am_i()

    def few(start, rows):
        for s in range(lay.n):
            row = 1 - a if lay.crosses(s, home) else a
            k = lay.window_of(p ^ s, row, home)
            outside, partner, halo = masks(place_refs, row, k, p, lay, start)
            for c in range(4):
                mine = jnp.where(halo, spread(own_halo[c, rows, :], lay), own[c, rows, :])
                theirs = jnp.where(halo, spread(prt_halo[c, rows, :], lay), prt[c, rows, :])
                if lay.crosses(s, home):
                    mine, theirs = theirs, mine
                value = jnp.where(partner, theirs, jnp.where(outside, 0.0, mine))
                out_refs[c // 2 * lay.n + s][c % 2, rows, :] = value

    by_rows(lay, few)


def spread(halo, lay):
    return halo if lay.t == 2 * lay.m else jnp.concatenate([halo, halo], axis=1)


def roll_half(x, lay):
    return pltpu.roll(x, lay.m, 1)


def kernel_strips(lay):
    t, m = lay.t, lay.m

    def body(own_ref, prt_ref, out_ref):
        a = lax.axis_index("ty")
        low = iota((lay.h, 2 * m), 1) < m
        for c in range(4):
            for row in (0, 1):

                @pl.when(a == row)
                def _(c=c, row=row):
                    cut = slice(t - 2 * m, t) if row == 0 else slice(0, 2 * m)
                    first, second = (own_ref, prt_ref) if row == 0 else (prt_ref, own_ref)
                    x0, x1 = first[c, :, cut], roll_half(second[c, :, cut], lay)
                    out_ref[c] = jnp.where(low, x1, x0) if row == 0 else jnp.where(low, x0, x1)

    return body


def kernel_pack(lay):
    m = lay.m

    def body(place_ref, other_ref, own_ref, prt_ref, mine_ref, theirs_ref, *outs):
        a, b, _ = where_am_i()
        blocks, own_halo_ref, prt_halo_ref = outs[: 2 * lay.n], *outs[2 * lay.n :]
        low = iota((lay.h, 2 * m), 1) < m
        keep = jnp.where(low, (b < lay.ntx - 1).astype(F32), (b > 0).astype(F32))
        for c in range(4):
            from_left = jnp.where(a == 0, mine_ref[c], theirs_ref[c])
            from_right = jnp.where(a == 0, theirs_ref[c], mine_ref[c])
            halo0 = jnp.where(low, from_right, from_left)
            halo1 = jnp.where(low, roll_half(from_right, lay), roll_half(from_left, lay))
            own_halo_ref[c] = jnp.where(keep > 0, jnp.where(a == 0, halo0, halo1), 0.0)
            prt_halo_ref[c] = jnp.where(keep > 0, jnp.where(a == 0, halo1, halo0), 0.0)
        pack_blocks((place_ref, other_ref), own_ref, own_halo_ref, prt_ref, prt_halo_ref, blocks, lay, False)

    return body


def move(target, *arrays):
    count = len(arrays)
    inward = target is pltpu.VMEM
    here, there = vmem(), pl.BlockSpec(memory_space=pl.ANY)

    def body(*refs):
        sources, targets, sems = refs[:count], refs[count : 2 * count], refs[2 * count]
        copies = [pltpu.make_async_copy(x, y, sems.at[i]) for i, (x, y) in enumerate(zip(sources, targets))]
        for copy in copies:
            copy.start()
        for copy in copies:
            copy.wait()

    return pl.pallas_call(
        body,
        out_shape=tuple(target(x.shape, x.dtype) for x in arrays),
        in_specs=[there if inward else here] * count,
        out_specs=tuple(here if inward else there for _ in arrays),
        scratch_shapes=[pltpu.SemaphoreType.DMA((count,))],
        compiler_params=pltpu.CompilerParams(vmem_limit_bytes=2 * 1024 * 1024),
    )(*[pltpu.with_memory_space_constraint(x, pltpu.HBM if inward else pltpu.VMEM) for x in arrays])


def series(z, first):
    terms = [(-1) ** i / math.factorial(2 * i + first) for i in range(8)]
    value = terms[-1]
    for term in terms[-2::-1]:
        value = value * z + term
    return value


def kernel_slab(phase_ref, slab_ref):
    y = 0.5 * phase_ref[...]
    z = y * y
    sine, cosine = series(z, 1) * y, series(z, 0)
    slab_ref[0] = 1.0 - 2.0 * sine * sine
    slab_ref[1] = 2.0 * sine * cosine


def kernel_probe(lay, home):
    def body(place_ref, light_ref, out_ref):
        a, _, p = where_am_i()
        k = jnp.clip(lay.window_of(p, a, home), 0, lay.slots - 1)
        down, along = ((place_ref[0, 0, i, k] + (lay.t - lay.m)) % lay.t for i in range(2))
        for c in range(2):
            out_ref[c] = pltpu.roll(pltpu.roll(light_ref[c], down, 0), along, 1)

    return body


def assemble(blocks, window_ref, lay):
    p = lax.axis_index("pos")
    for s in range(lay.n):
        start = pl.multiple_of((p ^ s) * lay.h, lay.h)
        for c in range(window_ref.shape[0]):
            window_ref[c, pl.ds(start, lay.h), :] = blocks[s][c]


def propagate(o1r, o1i, light_ref, slab_ref, tab):
    er, ei = cmul(light_ref[0], light_ref[1], o1r, o1i)
    sr, si = transform(er, ei, tab, False)
    sr, si = cmul(sr, si, slab_ref[0], slab_ref[1])
    return transform(sr, si, tab, True)


def live(count_ref, lay, home):
    a, _, p = where_am_i()
    k = lay.window_of(p, a, home)
    return (k >= 0) & (k < count_ref[0, 0])


def scatter(value, c, outs, lay):
    p = lax.axis_index("pos")
    for s in range(lay.n):
        outs[s][c] = value[pl.ds(pl.multiple_of((p ^ s) * lay.h, lay.h), lay.h), :]


def kernel_backward(lay):
    def body(count_ref, *refs):
        n = lay.n
        blocks, (between_ref, tab, meas_ref, moved_ref) = refs[:n], refs[n : n + 4]
        toward_ref, outs, window_ref, grad_ref = refs[n + 4], refs[n + 5 : 2 * n + 5], *refs[2 * n + 5 :]

        @pl.when(live(count_ref, lay, False))
        def _():
            assemble(blocks, window_ref, lay)
            br, bi = between_ref[0], between_ref[1]
            lr, li = cmul(br, bi, window_ref[0], window_ref[1])
            fr, fi = transform(lr, li, tab, False)
            seen = jnp.where(lax.axis_index("ty") == 0, meas_ref[0, 0, 0], moved_ref[0, 0, 0])
            keeping = 1.0 - seen / jnp.maximum(jnp.sqrt(fr * fr + fi * fi), magnitude_floor)
            kr, ki = transform(fr * keeping, fi * keeping, tab, True)
            toward_ref[0], toward_ref[1] = cmul(window_ref[0], -window_ref[1], kr, ki)
            grad_ref[0], grad_ref[1] = cmul(br, -bi, kr, ki)
            for c in range(2):
                scatter(grad_ref.at[c], c, outs, lay)

    return body


def kernel_final(lay):
    def body(count_ref, toward_ref, light_ref, slab_ref, tab, *refs):
        outs, grad_ref = refs[: lay.n], refs[lay.n]

        @pl.when(live(count_ref, lay, False))
        def _():
            sr, si = transform(toward_ref[0], toward_ref[1], tab, False)
            sr, si = cmul(sr, si, slab_ref[0], -slab_ref[1])
            ir, ii = transform(sr, si, tab, True)
            grad_ref[0], grad_ref[1] = cmul(light_ref[0], -light_ref[1], ir, ii)
            for c in range(2):
                scatter(grad_ref.at[c], c, outs, lay)

    return body


def kernel_collect(lay):
    t, m = lay.t, lay.m

    def body(place_ref, other_ref, count_ref, other_count_ref, *refs):
        n = lay.n
        blocks, mom_ref = refs[: 2 * n], refs[2 * n]
        own_ref, halo_ref = refs[2 * n + 1 :]
        a, _, p = where_am_i()
        low = iota((step(lay), 2 * m), 1) < m

        def few(start, few_rows):
            totals = [[momentum_rate * mom_ref[c, few_rows, :], jnp.zeros((step(lay), t), F32)] for c in range(4)]
            edges = [[jnp.zeros((step(lay), 2 * m), F32) for _ in range(2)] for _ in range(4)]
            for s in range(n):
                crosses = lay.crosses(s, False)
                row = 1 - a if crosses else a
                k = lay.window_of(p ^ s, row, False)
                valid = (k >= 0) & (k < (other_count_ref if crosses else count_ref)[0, 0])
                outside, partner, halo = masks((place_ref, other_ref), row, k, p, lay, start)
                inside, partner = ~outside & valid, partner & valid
                for i, rows in enumerate((partner, inside) if crosses else (inside, partner)):
                    for c in range(4):
                        g = jnp.where(rows, blocks[c // 2 * n + s][c % 2, few_rows, :], 0.0)
                        x = jnp.where(halo, g, 0.0)
                        totals[c][i] += jnp.where(halo, 0.0, g)
                        edges[c][i] += jnp.where(low, x[:, : 2 * m], x[:, t - 2 * m :])
            for c in range(4):
                for i in range(2):
                    own_ref[i, c, few_rows, :] = totals[c][i]
                    halo_ref[i, c, few_rows, :] = edges[c][i]

        by_rows(lay, few)

    return body


def kernel_strips_back(lay):
    t, m = lay.t, lay.m

    def body(own_ref, halo_ref, their_own_ref, their_halo_ref, sum_ref, halo_sum_ref, out_ref):
        a = lax.axis_index("ty")
        low = iota((lay.h, 2 * m), 1) < m
        for c in range(4):
            for i in range(2):
                sum_ref[i, c] = own_ref[i, c] + their_own_ref[1 - i, c]
                halo_sum_ref[i, c] = halo_ref[i, c] + their_halo_ref[1 - i, c]
        for row in (0, 1):

            @pl.when(a == row)
            def _(row=row):
                for tile in range(2):
                    i = tile ^ row
                    for c in range(4):
                        halo = halo_sum_ref[i, c]
                        if row == 0:
                            out_ref[tile, c] = jnp.where(low, halo, sum_ref[i, c, :, t - 2 * m :])
                        else:
                            out_ref[tile, c] = jnp.where(low, sum_ref[i, c, :, : 2 * m], halo)

    return body


def kernel_update(lay):
    m = lay.m

    def body(place_ref, obj_ref, prt_ref, obj_halo_ref, prt_halo_ref, sum_ref, halo_sum_ref, mine_ref, theirs_ref, *outs):
        n = lay.n
        new_ref, vel_ref, *blocks = outs[: 2 * n + 2]
        prt_new, own_halo, prt_halo = outs[2 * n + 2 :]
        a, b, _ = where_am_i()
        low = iota((lay.h, 2 * m), 1) < m
        not_first, not_last = b > 0, b < lay.ntx - 1
        keep = (low & not_last) | (~low & not_first)
        for i in range(2):
            tile = a if i == 0 else 1 - a
            for c in range(4):
                mine, theirs = mine_ref[tile, c], theirs_ref[tile, c]
                from_left = jnp.where(not_first, jnp.where(a == 0, mine, theirs), 0.0)
                from_right = jnp.where(not_last, jnp.where(a == 0, theirs, mine), 0.0)
                v = sum_ref[i, c] + jnp.concatenate(
                    [jnp.where(low, from_left, 0.0), jnp.where(low, 0.0, from_right)], axis=1
                )
                hv = halo_sum_ref[i, c] + jnp.where(low, from_right, from_left)
                obj, halo = (obj_ref, obj_halo_ref) if i == 0 else (prt_ref, prt_halo_ref)
                new, new_halo = (new_ref, own_halo) if i == 0 else (prt_new, prt_halo)
                if i == 0:
                    vel_ref[c] = v
                new[c] = obj[c] - step_length * v
                new_halo[c] = jnp.where(keep, halo[c] - step_length * hv, 0.0)
        pack_blocks((place_ref, place_ref), new_ref, own_halo, prt_new, prt_halo, blocks, lay, True)

    return body


def kernel_between(lay, home):
    def body(count_ref, *refs):
        n = lay.n
        blocks, (light_ref, slab_ref, tab), out_ref, window_ref = refs[:n], refs[n : n + 3], refs[n + 3], refs[n + 4]

        @pl.when(live(count_ref, lay, home))
        def _():
            assemble(blocks, window_ref, lay)
            out_ref[0], out_ref[1] = propagate(window_ref[0], window_ref[1], light_ref, slab_ref, tab)

    return body


def kernel_predict(lay):
    def body(count_ref, *refs):
        n = lay.n
        blocks, (between_ref, tab), out_ref, window_ref = refs[:n], refs[n : n + 2], refs[n + 2], refs[n + 3]
        used = live(count_ref, lay, True)

        @pl.when(used)
        def _():
            assemble(blocks, window_ref, lay)
            lr, li = cmul(between_ref[0], between_ref[1], window_ref[0], window_ref[1])
            fr, fi = transform(lr, li, tab, False)
            out_ref[0, 0, 0] = jnp.sqrt(fr * fr + fi * fi)

        @pl.when(jnp.logical_not(used))
        def _():
            out_ref[...] = jnp.zeros(out_ref.shape, F32)

    return body


def iteration(object_field, momentum, measured, illumination, slab_phase, offsets, entry_counts):
    lay = Layout(object_field, illumination, offsets)
    n, h, t, m = lay.n, lay.h, lay.t, lay.m
    own = object_field.reshape(4, h, t)
    offsets = offsets.transpose(0, 1, 3, 2)
    velocity_old = momentum.reshape(4, h, t)
    block, half_block, halo_shape = (4, h, t), (2, h, t), (4, h, 2 * m)
    tab = jnp.asarray(dft_tables(t))
    cores = lambda x: lax.ppermute(x, "ty", [(0, 1), (1, 0)])
    partner = cores(own)
    other_offsets = cores(offsets)
    other_counts = cores(entry_counts)
    (own,) = move(pltpu.VMEM, own)
    ntx = lay.ntx
    shift = [(b, b + 1) for b in range(ntx - 1)] + [(ntx - 1, 2 * ntx - 1)]
    shift += [(ntx + b + 1, ntx + b) for b in range(ntx - 1)] + [(ntx, 0)]
    columns = lambda x: lax.ppermute(x, ("ty", "tx"), shift)

    def exchange(values, pairs_of):
        got = [values[0]]
        for s in range(1, n):
            got.append(lax.ppermute(values[s], ("ty", "pos"), complete(pairs_of(s), n)))
        return got

    low, high = range(lay.half), range(lay.half, n)
    pairs = [(n + p, n + p + lay.half) for p in low] + [(p, p - lay.half) for p in high]
    pairs += [(p, n + p) for p in low] + [(n + p, p) for p in high]
    moved = lax.ppermute(measured, ("ty", "pos"), pairs)
    velocity_old, measured, illumination, slab_phase, tab = move(
        pltpu.VMEM, velocity_old, measured, illumination, slab_phase, tab
    )
    (slab,) = call(kernel_slab, [(2, t, t)], [slab_phase])
    lights = []
    for home in range(2):
        (light,) = call(kernel_probe(lay, bool(home)), [(2, t, t)], [offsets, illumination], 1)
        lights.append(light)
    light, light_home = lights
    (strips,) = call(kernel_strips(lay), [halo_shape], [own, partner])
    strips = columns(strips)
    strips_other = cores(strips)
    *blocks, own_halo, partner_halo = call(
        kernel_pack(lay),
        [half_block] * (2 * n) + [halo_shape] * 2,
        [offsets, other_offsets, own, partner, strips, strips_other],
        2,
    )
    first = exchange(blocks[:n], lambda s: lay.inward(s, False))
    second = exchange(blocks[n:], lambda s: lay.inward(s, False))
    half_window = pltpu.VMEM((2, t, t), F32)

    def propagated(first, light, home):
        (between,) = call(
            kernel_between(lay, home), [(2, t, t)], [entry_counts, *first, light, slab, tab], 1, [half_window], limit=24
        )
        return between

    between = propagated(first, light, False)
    toward, *terms_second = call(
        kernel_backward(lay),
        [(2, t, t)] + [half_block] * n,
        [entry_counts, *second, between, tab, measured, moved],
        1,
        [half_window, half_window],
        limit=24,
    )
    parts_second = exchange(terms_second, lay.outward)
    terms_first = call(
        kernel_final(lay), [half_block] * n, [entry_counts, toward, light, slab, tab], 1, [half_window], limit=24
    )
    parts_first = exchange(terms_first, lay.outward)
    sums, halos = call(
        kernel_collect(lay),
        [(2, *block), (2, *halo_shape)],
        [offsets, other_offsets, entry_counts, other_counts, *parts_first, *parts_second, velocity_old],
        4,
    )
    sums, halos, strips = call(
        kernel_strips_back(lay),
        [(2, *block), (2, *halo_shape), (2, *halo_shape)],
        [sums, halos, cores(sums), cores(halos)],
    )
    strips = columns(strips)
    updated, velocity, *rest = call(
        kernel_update(lay),
        [block] * 2 + [half_block] * (2 * n),
        [offsets, own, partner, own_halo, partner_halo, sums, halos, strips, cores(strips)],
        1,
        [pltpu.VMEM(block, F32), pltpu.VMEM(halo_shape, F32), pltpu.VMEM(halo_shape, F32)],
    )
    first = exchange(rest[:n], lambda s: lay.inward(s, True))
    second = exchange(rest[n : 2 * n], lambda s: lay.inward(s, True))
    updated, velocity = move(pltpu.HBM, updated, velocity)
    between = propagated(first, light_home, True)
    (amplitudes,) = call(
        kernel_predict(lay),
        [measured.shape],
        [entry_counts, *second, between, tab],
        1,
        [half_window],
        limit=24,
        last=True,
    )
    return (
        updated.reshape(object_field.shape),
        velocity.reshape(momentum.shape),
        amplitudes,
    )


def solution(mesh):
    placed = (
        P(None, None, ("ty", "pos"), "tx"),
        P(None, None, ("ty", "pos"), "tx"),
        P("ty", "tx", "pos", None, None),
        P(),
        P(),
        P("ty", "tx", None, None),
        P("ty", "tx"),
    )
    return jax.shard_map(
        iteration,
        mesh=mesh,
        in_specs=placed,
        out_specs=(
            P(None, None, ("ty", "pos"), "tx"),
            P(None, None, ("ty", "pos"), "tx"),
            P("ty", "tx", "pos", None, None),
        ),
        check_vma=False,
    )
```

```python
import math

import jax
import jax.numpy as jnp
import numpy as np
from jax import lax
from jax.experimental import pallas as pl
from jax.experimental.pallas import tpu as pltpu
from jax.sharding import PartitionSpec as P


magnitude_floor = 0.5
momentum_rate = 0.9
step_length = 0.05
F32 = jnp.float32
BF16 = jnp.bfloat16


def vmem():
    return pl.BlockSpec(memory_space=pltpu.VMEM)


def smem():
    return pl.BlockSpec(memory_space=pltpu.SMEM)


def call(body, outs, args, scalars=0, scratch=(), limit=8, last=False):
    specs = [smem()] * scalars + [vmem()] * (len(args) - scalars)
    placed = [pltpu.with_memory_space_constraint(x, pltpu.VMEM) for x in args[scalars:]]
    return pl.pallas_call(
        body,
        out_shape=tuple((jax.ShapeDtypeStruct if last else pltpu.VMEM)(s, F32) for s in outs),
        in_specs=specs,
        out_specs=tuple(vmem() for _ in outs),
        scratch_shapes=list(scratch),
        compiler_params=pltpu.CompilerParams(vmem_limit_bytes=limit * 1024 * 1024),
    )(*args[:scalars], *placed)


def split_table(values):
    high = values.astype(jnp.bfloat16)
    low = (values - high.astype(np.float64)).astype(jnp.bfloat16)
    return high, low


def dft_tables(length):
    index = np.arange(length)
    angles = (index[:, None] * index[None, :] % length) * (2.0 * math.pi / length)
    cosine, sine = np.cos(angles) / math.sqrt(length), np.sin(angles) / math.sqrt(length)
    parts = [part for t in (cosine, cosine + sine, cosine - sine) for part in split_table(t)]
    return np.stack(parts)


def iota(shape, dim):
    return lax.broadcasted_iota(jnp.int32, shape, dim)


def split(value):
    high = value.astype(BF16)
    return high, (value - high.astype(F32)).astype(BF16)


def dot(left, right):
    return jnp.dot(left, right, preferred_element_type=F32)


def mul3(left, right):
    return dot(left[0], right[0]) + dot(left[0], right[1]) + dot(left[1], right[0])


def transform(real, imag, tab, inverse):
    cos = (tab[0], tab[1])
    plus, minus = ((tab[4], tab[5]), (tab[2], tab[3])) if inverse else ((tab[2], tab[3]), (tab[4], tab[5]))
    both = mul3(split(real + imag), cos)
    right_imag = both - mul3(split(real), plus)
    left_low = mul3(minus, split(right_imag))
    right_real = both - mul3(split(imag), minus)
    both = mul3(cos, split(right_real + right_imag))
    return both - left_low, both - mul3(plus, split(right_real))


def cmul(ar, ai, br, bi):
    return ar * br - ai * bi, ar * bi + ai * br


class Layout:
    def __init__(self, object_field, illumination, offsets):
        self.n = lax.axis_size("pos")
        self.ntx = lax.axis_size("tx")
        self.nty = lax.axis_size("ty")
        self.h = object_field.shape[2]
        self.t = object_field.shape[3]
        self.m = illumination.shape[-1] // 4
        self.slots = offsets.shape[2]
        self.half = self.n // 2
        assert self.nty == 2 and self.slots == self.n and self.n & (self.n - 1) == 0
        assert self.t == illumination.shape[-1] == self.n * self.h == 4 * self.m

    def window_of(self, device, row, home):
        return device if home else device - row * self.half

    def holds(self, device, row, home):
        return 0 <= self.window_of(device, row, home) < self.half

    def crosses(self, s, home):
        return not home and 0 < s < self.half

    def inward(self, s, home):
        n = self.n
        core = (lambda a: 1 - a) if self.crosses(s, home) else (lambda a: a)
        return [(core(a) * n + p, a * n + (p ^ s)) for a in range(2) for p in range(n) if self.holds(p ^ s, a, home)]

    def outward(self, s):
        return [(d, o) for o, d in self.inward(s, False)]


def complete(pairs, n):
    sources, targets = {x for x, _ in pairs}, {y for _, y in pairs}
    other = lambda x: (x + n) % (2 * n)
    extra = [(x, other(x)) for x in range(2 * n) if x not in sources and other(x) not in targets]
    return pairs + extra if len(pairs) + len(extra) == 2 * n else pairs


def where_am_i():
    return lax.axis_index("ty"), lax.axis_index("tx"), lax.axis_index("pos")


def by_rows(lay, body, size):
    size = min(size, lay.h)
    for start in range(0, lay.h, size):
        body(start, slice(start, start + size))


def masks(place_refs, a, k, p, lay, few):
    h, t, m = lay.h, lay.t, lay.m
    k = jnp.clip(k, 0, lay.slots - 1)
    mine = a == lax.axis_index("ty")
    top, left = (jnp.where(mine, place_refs[0][0, 0, i, k], place_refs[1][0, 0, i, k]) - m for i in range(2))
    rows = iota((few.stop - few.start, t), 0) + (p * h + few.start)
    cols = iota((few.stop - few.start, t), 1)
    reaches = ((p * h + h > top + t) & (a == 1)) | ((p * h < top) & (a == 0))
    above = rows >= top + t
    below = rows < top
    outside = above | below
    partner = (above & (a == 1)) | (below & (a == 0))
    halo = (cols >= left + t) | (cols < left)
    return outside, partner, halo, reaches


def pack_blocks(place_refs, own, own_halo, prt, prt_halo, out_refs, lay, home):
    a, _, p = where_am_i()

    def few(_, rows):
        for s in range(lay.n):
            row = 1 - a if lay.crosses(s, home) else a
            k = lay.window_of(p ^ s, row, home)
            outside, partner, halo, _ = masks(place_refs, row, k, p, lay, rows)
            for c in range(4):
                mine = jnp.where(halo, spread(own_halo[c, rows, :], lay), own[c, rows, :])
                theirs = jnp.where(halo, spread(prt_halo[c, rows, :], lay), prt[c, rows, :])
                if lay.crosses(s, home):
                    mine, theirs = theirs, mine
                value = jnp.where(partner, theirs, jnp.where(outside, 0.0, mine))
                out_refs[c // 2 * lay.n + s][c % 2, rows, :] = value

    by_rows(lay, few, 8 if home else lay.h)


def spread(halo, lay):
    return halo if lay.t == 2 * lay.m else jnp.concatenate([halo, halo], axis=1)


def roll_half(x, lay):
    return pltpu.roll(x, lay.m, 1)


def kernel_strips(lay):
    t, m = lay.t, lay.m

    def body(own_ref, prt_ref, out_ref):
        a = lax.axis_index("ty")
        low = iota((lay.h, 2 * m), 1) < m
        for c in range(4):
            for row in (0, 1):

                @pl.when(a == row)
                def _(c=c, row=row):
                    cut = slice(t - 2 * m, t) if row == 0 else slice(0, 2 * m)
                    first, second = (own_ref, prt_ref) if row == 0 else (prt_ref, own_ref)
                    x0, x1 = first[c, :, cut], roll_half(second[c, :, cut], lay)
                    out_ref[c] = jnp.where(low, x1, x0) if row == 0 else jnp.where(low, x0, x1)

    return body


def kernel_pack(lay):
    m = lay.m

    def body(place_ref, other_ref, own_ref, prt_ref, mine_ref, theirs_ref, *outs):
        a, b, _ = where_am_i()
        blocks, own_halo_ref, prt_halo_ref = outs[: 2 * lay.n], *outs[2 * lay.n :]
        low = iota((lay.h, 2 * m), 1) < m
        keep = jnp.where(low, (b < lay.ntx - 1).astype(F32), (b > 0).astype(F32))
        for c in range(4):
            from_left = jnp.where(a == 0, mine_ref[c], theirs_ref[c])
            from_right = jnp.where(a == 0, theirs_ref[c], mine_ref[c])
            halo0 = jnp.where(low, from_right, from_left)
            halo1 = jnp.where(low, roll_half(from_right, lay), roll_half(from_left, lay))
            own_halo_ref[c] = jnp.where(keep > 0, jnp.where(a == 0, halo0, halo1), 0.0)
            prt_halo_ref[c] = jnp.where(keep > 0, jnp.where(a == 0, halo1, halo0), 0.0)
        pack_blocks((place_ref, other_ref), own_ref, own_halo_ref, prt_ref, prt_halo_ref, blocks, lay, False)

    return body


def move(target, *arrays):
    count = len(arrays)
    inward = target is pltpu.VMEM
    here, there = vmem(), pl.BlockSpec(memory_space=pl.ANY)

    def body(*refs):
        sources, targets, sems = refs[:count], refs[count : 2 * count], refs[2 * count]
        copies = [pltpu.make_async_copy(x, y, sems.at[i]) for i, (x, y) in enumerate(zip(sources, targets))]
        for copy in copies:
            copy.start()
        for copy in copies:
            copy.wait()

    return pl.pallas_call(
        body,
        out_shape=tuple(target(x.shape, x.dtype) for x in arrays),
        in_specs=[there if inward else here] * count,
        out_specs=tuple(here if inward else there for _ in arrays),
        scratch_shapes=[pltpu.SemaphoreType.DMA((count,))],
        compiler_params=pltpu.CompilerParams(vmem_limit_bytes=2 * 1024 * 1024),
    )(*[pltpu.with_memory_space_constraint(x, pltpu.HBM if inward else pltpu.VMEM) for x in arrays])


def series(z, first):
    terms = [(-1) ** i / math.factorial(2 * i + first) for i in range(8)]
    value = terms[-1]
    for term in terms[-2::-1]:
        value = value * z + term
    return value


def kernel_slab(phase_ref, slab_ref):
    y = 0.5 * phase_ref[...]
    z = y * y
    sine, cosine = series(z, 1) * y, series(z, 0)
    slab_ref[0] = 1.0 - 2.0 * sine * sine
    slab_ref[1] = 2.0 * sine * cosine


def kernel_probe(lay, home):
    def body(place_ref, light_ref, out_ref):
        a, _, p = where_am_i()
        k = jnp.clip(lay.window_of(p, a, home), 0, lay.slots - 1)
        down, along = ((place_ref[0, 0, i, k] + (lay.t - lay.m)) % lay.t for i in range(2))
        for c in range(2):
            out_ref[c] = pltpu.roll(pltpu.roll(light_ref[c], down, 0), along, 1)

    return body


def assemble(blocks, window_ref, lay):
    p = lax.axis_index("pos")
    for s in range(lay.n):
        start = pl.multiple_of((p ^ s) * lay.h, lay.h)
        for c in range(window_ref.shape[0]):
            window_ref[c, pl.ds(start, lay.h), :] = blocks[s][c]


def propagate(o1r, o1i, light_ref, slab_ref, tab):
    er, ei = cmul(light_ref[0], light_ref[1], o1r, o1i)
    sr, si = transform(er, ei, tab, False)
    sr, si = cmul(sr, si, slab_ref[0], slab_ref[1])
    return transform(sr, si, tab, True)


def live(count_ref, lay, home):
    a, _, p = where_am_i()
    k = lay.window_of(p, a, home)
    return (k >= 0) & (k < count_ref[0, 0])


def scatter(value, c, outs, lay):
    p = lax.axis_index("pos")
    for s in range(lay.n):
        outs[s][c] = value[pl.ds(pl.multiple_of((p ^ s) * lay.h, lay.h), lay.h), :]


def kernel_backward(lay):
    def body(count_ref, *refs):
        n = lay.n
        blocks, (between_ref, tab, meas_ref, moved_ref) = refs[:n], refs[n : n + 4]
        toward_ref, outs, window_ref, grad_ref = refs[n + 4], refs[n + 5 : 2 * n + 5], *refs[2 * n + 5 :]

        used = live(count_ref, lay, False)

        @pl.when(used)
        def _():
            assemble(blocks, window_ref, lay)
            br, bi = between_ref[0], between_ref[1]
            lr, li = cmul(br, bi, window_ref[0], window_ref[1])
            fr, fi = transform(lr, li, tab, False)
            seen = jnp.where(lax.axis_index("ty") == 0, meas_ref[0, 0, 0], moved_ref[0, 0, 0])
            keeping = 1.0 - seen / jnp.maximum(jnp.sqrt(fr * fr + fi * fi), magnitude_floor)
            kr, ki = transform(fr * keeping, fi * keeping, tab, True)
            toward_ref[0], toward_ref[1] = cmul(window_ref[0], -window_ref[1], kr, ki)
            grad_ref[0], grad_ref[1] = cmul(br, -bi, kr, ki)
            for c in range(2):
                scatter(grad_ref.at[c], c, outs, lay)

        @pl.when(jnp.logical_not(used))
        def _():
            for out in outs:
                out[...] = jnp.zeros(out.shape, F32)

    return body


def kernel_final(lay):
    def body(count_ref, toward_ref, light_ref, slab_ref, tab, *refs):
        outs, grad_ref = refs[: lay.n], refs[lay.n]
        used = live(count_ref, lay, False)

        @pl.when(used)
        def _():
            sr, si = transform(toward_ref[0], toward_ref[1], tab, False)
            sr, si = cmul(sr, si, slab_ref[0], -slab_ref[1])
            ir, ii = transform(sr, si, tab, True)
            grad_ref[0], grad_ref[1] = cmul(light_ref[0], -light_ref[1], ir, ii)
            for c in range(2):
                scatter(grad_ref.at[c], c, outs, lay)

        @pl.when(jnp.logical_not(used))
        def _():
            for out in outs:
                out[...] = jnp.zeros(out.shape, F32)

    return body


def kernel_collect(lay):
    t, m = lay.t, lay.m

    def body(place_ref, other_ref, *refs):
        n = lay.n
        blocks, mom_ref = refs[: 2 * n], refs[2 * n]
        own_ref, halo_ref = refs[2 * n + 1 :]
        a, _, p = where_am_i()
        low = iota((lay.h, 2 * m), 1) < m
        own_ref[0] = momentum_rate * mom_ref[...]
        own_ref[1] = jnp.zeros(own_ref.shape[1:], F32)
        halo_ref[...] = jnp.zeros(halo_ref.shape, F32)
        for s in range(n):
            crosses = lay.crosses(s, False)
            row = 1 - a if crosses else a
            k = lay.window_of(p ^ s, row, False)
            valid = (k >= 0) & (k < lay.half)
            cells = lambda row=row, k=k: masks((place_ref, other_ref), row, k, p, lay, slice(0, lay.h))
            reaches = cells()[3]

            def add(i, rows, halo, s=s):
                inner, left, right = rows & ~halo, (rows & halo)[:, : 2 * m] & low, (rows & halo)[:, t - 2 * m :] & ~low
                for c in range(4):
                    g = blocks[c // 2 * n + s][c % 2]
                    own_ref[i, c] += jnp.where(inner, g, 0.0)
                    halo_ref[i, c] += jnp.where(left, g[:, : 2 * m], jnp.where(right, g[:, t - 2 * m :], 0.0))

            @pl.when(valid)
            def _(i=int(crosses), cells=cells, add=add):
                outside, _, halo, _ = cells()
                add(i, ~outside, halo)

            @pl.when(valid & reaches)
            def _(i=1 - int(crosses), cells=cells, add=add):
                _, partner, halo, _ = cells()
                add(i, partner, halo)

    return body


def kernel_strips_back(lay):
    t, m = lay.t, lay.m

    def body(own_ref, halo_ref, their_own_ref, their_halo_ref, sum_ref, halo_sum_ref, out_ref):
        a = lax.axis_index("ty")
        low = iota((lay.h, 2 * m), 1) < m
        for c in range(4):
            for i in range(2):
                sum_ref[i, c] = own_ref[i, c] + their_own_ref[1 - i, c]
                halo_sum_ref[i, c] = halo_ref[i, c] + their_halo_ref[1 - i, c]
        for row in (0, 1):

            @pl.when(a == row)
            def _(row=row):
                for tile in range(2):
                    i = tile ^ row
                    for c in range(4):
                        halo = halo_sum_ref[i, c]
                        if row == 0:
                            out_ref[tile, c] = jnp.where(low, halo, sum_ref[i, c, :, t - 2 * m :])
                        else:
                            out_ref[tile, c] = jnp.where(low, sum_ref[i, c, :, : 2 * m], halo)

    return body


def kernel_update(lay):
    m = lay.m

    def body(place_ref, obj_ref, prt_ref, obj_halo_ref, prt_halo_ref, sum_ref, halo_sum_ref, mine_ref, theirs_ref, *outs):
        n = lay.n
        new_ref, vel_ref, *blocks = outs[: 2 * n + 2]
        prt_new, own_halo, prt_halo = outs[2 * n + 2 :]
        a, b, _ = where_am_i()
        low = iota((lay.h, 2 * m), 1) < m
        not_first, not_last = b > 0, b < lay.ntx - 1
        keep = (low & not_last) | (~low & not_first)
        for i in range(2):
            tile = a if i == 0 else 1 - a
            for c in range(4):
                mine, theirs = mine_ref[tile, c], theirs_ref[tile, c]
                from_left = jnp.where(not_first, jnp.where(a == 0, mine, theirs), 0.0)
                from_right = jnp.where(not_last, jnp.where(a == 0, theirs, mine), 0.0)
                v = sum_ref[i, c] + jnp.concatenate(
                    [jnp.where(low, from_left, 0.0), jnp.where(low, 0.0, from_right)], axis=1
                )
                hv = halo_sum_ref[i, c] + jnp.where(low, from_right, from_left)
                obj, halo = (obj_ref, obj_halo_ref) if i == 0 else (prt_ref, prt_halo_ref)
                new, new_halo = (new_ref, own_halo) if i == 0 else (prt_new, prt_halo)
                if i == 0:
                    vel_ref[c] = v
                new[c] = obj[c] - step_length * v
                new_halo[c] = jnp.where(keep, halo[c] - step_length * hv, 0.0)
        pack_blocks((place_ref, place_ref), new_ref, own_halo, prt_new, prt_halo, blocks, lay, True)

    return body


def kernel_between(lay, home):
    def body(count_ref, *refs):
        n = lay.n
        blocks, (light_ref, slab_ref, tab), out_ref, window_ref = refs[:n], refs[n : n + 3], refs[n + 3], refs[n + 4]

        @pl.when(live(count_ref, lay, home))
        def _():
            assemble(blocks, window_ref, lay)
            out_ref[0], out_ref[1] = propagate(window_ref[0], window_ref[1], light_ref, slab_ref, tab)

    return body


def kernel_predict(lay):
    def body(count_ref, *refs):
        n = lay.n
        blocks, (between_ref, tab), out_ref, window_ref = refs[:n], refs[n : n + 2], refs[n + 2], refs[n + 3]
        used = live(count_ref, lay, True)

        @pl.when(used)
        def _():
            assemble(blocks, window_ref, lay)
            lr, li = cmul(between_ref[0], between_ref[1], window_ref[0], window_ref[1])
            fr, fi = transform(lr, li, tab, False)
            out_ref[0, 0, 0] = jnp.sqrt(fr * fr + fi * fi)

        @pl.when(jnp.logical_not(used))
        def _():
            out_ref[...] = jnp.zeros(out_ref.shape, F32)

    return body


def iteration(object_field, momentum, measured, illumination, slab_phase, offsets, entry_counts):
    lay = Layout(object_field, illumination, offsets)
    n, h, t, m = lay.n, lay.h, lay.t, lay.m
    own = object_field.reshape(4, h, t)
    offsets = offsets.transpose(0, 1, 3, 2)
    velocity_old = momentum.reshape(4, h, t)
    block, half_block, halo_shape = (4, h, t), (2, h, t), (4, h, 2 * m)
    tab = jnp.asarray(dft_tables(t))
    cores = lambda x: lax.ppermute(x, "ty", [(0, 1), (1, 0)])
    partner = cores(own)
    other_offsets = cores(offsets)
    (own,) = move(pltpu.VMEM, own)
    ntx = lay.ntx
    shift = [(b, b + 1) for b in range(ntx - 1)] + [(ntx - 1, 2 * ntx - 1)]
    shift += [(ntx + b + 1, ntx + b) for b in range(ntx - 1)] + [(ntx, 0)]
    columns = lambda x: lax.ppermute(x, ("ty", "tx"), shift)

    def exchange(values, pairs_of):
        got = [values[0]]
        for s in range(1, n):
            got.append(lax.ppermute(values[s], ("ty", "pos"), complete(pairs_of(s), n)))
        return got

    low, high = range(lay.half), range(lay.half, n)
    pairs = [(n + p, n + p + lay.half) for p in low] + [(p, p - lay.half) for p in high]
    pairs += [(p, n + p) for p in low] + [(n + p, p) for p in high]
    moved = lax.ppermute(measured, ("ty", "pos"), pairs)
    velocity_old, measured, illumination, slab_phase, tab = move(
        pltpu.VMEM, velocity_old, measured, illumination, slab_phase, tab
    )
    (slab,) = call(kernel_slab, [(2, t, t)], [slab_phase])
    lights = []
    for home in range(2):
        (light,) = call(kernel_probe(lay, bool(home)), [(2, t, t)], [offsets, illumination], 1)
        lights.append(light)
    light, light_home = lights
    (strips,) = call(kernel_strips(lay), [halo_shape], [own, partner])
    strips = columns(strips)
    strips_other = cores(strips)
    *blocks, own_halo, partner_halo = call(
        kernel_pack(lay),
        [half_block] * (2 * n) + [halo_shape] * 2,
        [offsets, other_offsets, own, partner, strips, strips_other],
        2,
    )
    first = exchange(blocks[:n], lambda s: lay.inward(s, False))
    second = exchange(blocks[n:], lambda s: lay.inward(s, False))
    half_window = pltpu.VMEM((2, t, t), F32)

    def propagated(first, light, home):
        (between,) = call(
            kernel_between(lay, home), [(2, t, t)], [entry_counts, *first, light, slab, tab], 1, [half_window], limit=24
        )
        return between

    between = propagated(first, light, False)
    toward, *terms_second = call(
        kernel_backward(lay),
        [(2, t, t)] + [half_block] * n,
        [entry_counts, *second, between, tab, measured, moved],
        1,
        [half_window, half_window],
        limit=24,
    )
    parts_second = exchange(terms_second, lay.outward)
    terms_first = call(
        kernel_final(lay), [half_block] * n, [entry_counts, toward, light, slab, tab], 1, [half_window], limit=24
    )
    parts_first = exchange(terms_first, lay.outward)
    sums, halos = call(
        kernel_collect(lay),
        [(2, *block), (2, *halo_shape)],
        [offsets, other_offsets, *parts_first, *parts_second, velocity_old],
        2,
    )
    sums, halos, strips = call(
        kernel_strips_back(lay),
        [(2, *block), (2, *halo_shape), (2, *halo_shape)],
        [sums, halos, cores(sums), cores(halos)],
    )
    strips = columns(strips)
    updated, velocity, *rest = call(
        kernel_update(lay),
        [block] * 2 + [half_block] * (2 * n),
        [offsets, own, partner, own_halo, partner_halo, sums, halos, strips, cores(strips)],
        1,
        [pltpu.VMEM(block, F32), pltpu.VMEM(halo_shape, F32), pltpu.VMEM(halo_shape, F32)],
    )
    first = exchange(rest[:n], lambda s: lay.inward(s, True))
    second = exchange(rest[n : 2 * n], lambda s: lay.inward(s, True))
    updated, velocity = move(pltpu.HBM, updated, velocity)
    between = propagated(first, light_home, True)
    (amplitudes,) = call(
        kernel_predict(lay),
        [measured.shape],
        [entry_counts, *second, between, tab],
        1,
        [half_window],
        limit=24,
        last=True,
    )
    return (
        updated.reshape(object_field.shape),
        velocity.reshape(momentum.shape),
        amplitudes,
    )


def solution(mesh):
    placed = (
        P(None, None, ("ty", "pos"), "tx"),
        P(None, None, ("ty", "pos"), "tx"),
        P("ty", "tx", "pos", None, None),
        P(),
        P(),
        P("ty", "tx", None, None),
        P("ty", "tx"),
    )
    return jax.shard_map(
        iteration,
        mesh=mesh,
        in_specs=placed,
        out_specs=(
            P(None, None, ("ty", "pos"), "tx"),
            P(None, None, ("ty", "pos"), "tx"),
            P("ty", "tx", "pos", None, None),
        ),
        check_vma=False,
    )
```

```python
import math

import jax
import jax.numpy as jnp
import numpy as np
from jax import lax
from jax.experimental import pallas as pl
from jax.experimental.pallas import tpu as pltpu
from jax.sharding import PartitionSpec as P


magnitude_floor = 0.5
momentum_rate = 0.9
step_length = 0.05
F32 = jnp.float32
BF16 = jnp.bfloat16


def vmem():
    return pl.BlockSpec(memory_space=pltpu.VMEM)


def smem():
    return pl.BlockSpec(memory_space=pltpu.SMEM)


def call(body, outs, args, scalars=0, scratch=(), limit=8, last=False):
    specs = [smem()] * scalars + [vmem()] * (len(args) - scalars)
    placed = [pltpu.with_memory_space_constraint(x, pltpu.VMEM) for x in args[scalars:]]
    return pl.pallas_call(
        body,
        out_shape=tuple((jax.ShapeDtypeStruct if last else pltpu.VMEM)(s, F32) for s in outs),
        in_specs=specs,
        out_specs=tuple(vmem() for _ in outs),
        scratch_shapes=list(scratch),
        compiler_params=pltpu.CompilerParams(vmem_limit_bytes=limit * 1024 * 1024),
    )(*args[:scalars], *placed)


def split_table(values):
    high = values.astype(jnp.bfloat16)
    low = (values - high.astype(np.float64)).astype(jnp.bfloat16)
    return high, low


def dft_tables(length):
    index = np.arange(length)
    angles = (index[:, None] * index[None, :] % length) * (2.0 * math.pi / length)
    cosine, sine = np.cos(angles) / math.sqrt(length), np.sin(angles) / math.sqrt(length)
    parts = [part for t in (cosine, cosine + sine, cosine - sine) for part in split_table(t)]
    return np.stack(parts)


def iota(shape, dim):
    return lax.broadcasted_iota(jnp.int32, shape, dim)


def split(value):
    high = value.astype(BF16)
    return high, (value - high.astype(F32)).astype(BF16)


def dot(left, right):
    return jnp.dot(left, right, preferred_element_type=F32)


def mul3(left, right):
    return dot(left[0], right[0]) + dot(left[0], right[1]) + dot(left[1], right[0])


def transform(real, imag, tab, inverse):
    cos = (tab[0], tab[1])
    plus, minus = ((tab[4], tab[5]), (tab[2], tab[3])) if inverse else ((tab[2], tab[3]), (tab[4], tab[5]))
    both = mul3(split(real + imag), cos)
    right_imag = both - mul3(split(real), plus)
    left_low = mul3(minus, split(right_imag))
    right_real = both - mul3(split(imag), minus)
    both = mul3(cos, split(right_real + right_imag))
    return both - left_low, both - mul3(plus, split(right_real))


def cmul(ar, ai, br, bi):
    return ar * br - ai * bi, ar * bi + ai * br


class Layout:
    def __init__(self, object_field, illumination, offsets):
        self.n = lax.axis_size("pos")
        self.ntx = lax.axis_size("tx")
        self.nty = lax.axis_size("ty")
        self.h = object_field.shape[2]
        self.t = object_field.shape[3]
        self.m = illumination.shape[-1] // 4
        self.slots = offsets.shape[2]
        self.half = self.n // 2
        assert self.nty == 2 and self.slots == self.n and self.n & (self.n - 1) == 0
        assert self.t == illumination.shape[-1] == self.n * self.h == 4 * self.m

    def window_of(self, device, row, home):
        return device if home else device - row * self.half

    def holds(self, device, row, home):
        return 0 <= self.window_of(device, row, home) < self.half

    def crosses(self, s, home):
        return not home and 0 < s < self.half

    def inward(self, s, home):
        n = self.n
        core = (lambda a: 1 - a) if self.crosses(s, home) else (lambda a: a)
        return [(core(a) * n + p, a * n + (p ^ s)) for a in range(2) for p in range(n) if self.holds(p ^ s, a, home)]

    def outward(self, s):
        return [(d, o) for o, d in self.inward(s, False)]


def complete(pairs, n):
    sources, targets = {x for x, _ in pairs}, {y for _, y in pairs}
    other = lambda x: (x + n) % (2 * n)
    extra = [(x, other(x)) for x in range(2 * n) if x not in sources and other(x) not in targets]
    return pairs + extra if len(pairs) + len(extra) == 2 * n else pairs


def where_am_i():
    return lax.axis_index("ty"), lax.axis_index("tx"), lax.axis_index("pos")


def by_rows(lay, body, size):
    size = min(size, lay.h)
    for start in range(0, lay.h, size):
        body(start, slice(start, start + size))


def masks(place_refs, a, k, p, lay, few):
    h, t, m = lay.h, lay.t, lay.m
    k = jnp.clip(k, 0, lay.slots - 1)
    mine = a == lax.axis_index("ty")
    top, left = (jnp.where(mine, place_refs[0][0, 0, i, k], place_refs[1][0, 0, i, k]) - m for i in range(2))
    rows = iota((few.stop - few.start, t), 0) + (p * h + few.start)
    cols = iota((few.stop - few.start, t), 1)
    reaches = ((p * h + h > top + t) & (a == 1)) | ((p * h < top) & (a == 0))
    above = rows >= top + t
    below = rows < top
    outside = above | below
    partner = (above & (a == 1)) | (below & (a == 0))
    halo = (cols >= left + t) | (cols < left)
    return outside, partner, halo, reaches


def pack_blocks(place_refs, own, own_halo, prt, prt_halo, out_refs, lay, home, parts):
    a, _, p = where_am_i()

    def few(_, rows):
        for s in range(lay.n):
            row = 1 - a if lay.crosses(s, home) else a
            k = lay.window_of(p ^ s, row, home)
            outside, partner, halo, _ = masks(place_refs, row, k, p, lay, rows)
            for c in parts:
                mine = jnp.where(halo, spread(own_halo[c, rows, :], lay), own[c, rows, :])
                theirs = jnp.where(halo, spread(prt_halo[c, rows, :], lay), prt[c, rows, :])
                if lay.crosses(s, home):
                    mine, theirs = theirs, mine
                value = jnp.where(partner, theirs, jnp.where(outside, 0.0, mine))
                out_refs[(c - parts[0]) // 2 * lay.n + s][c % 2, rows, :] = value

    by_rows(lay, few, 8 if home else lay.h)


def spread(halo, lay):
    return halo if lay.t == 2 * lay.m else jnp.concatenate([halo, halo], axis=1)


def roll_half(x, lay):
    return pltpu.roll(x, lay.m, 1)


def kernel_strips(lay):
    t, m = lay.t, lay.m

    def body(own_ref, prt_ref, out_ref):
        a = lax.axis_index("ty")
        low = iota((lay.h, 2 * m), 1) < m
        for c in range(4):
            for row in (0, 1):

                @pl.when(a == row)
                def _(c=c, row=row):
                    cut = slice(t - 2 * m, t) if row == 0 else slice(0, 2 * m)
                    first, second = (own_ref, prt_ref) if row == 0 else (prt_ref, own_ref)
                    x0, x1 = first[c, :, cut], roll_half(second[c, :, cut], lay)
                    out_ref[c] = jnp.where(low, x1, x0) if row == 0 else jnp.where(low, x0, x1)

    return body


def kernel_pack(lay):
    m = lay.m

    def body(place_ref, other_ref, own_ref, prt_ref, mine_ref, theirs_ref, *outs):
        a, b, _ = where_am_i()
        blocks, own_halo_ref, prt_halo_ref = outs[: lay.n], *outs[lay.n :]
        low = iota((lay.h, 2 * m), 1) < m
        keep = jnp.where(low, (b < lay.ntx - 1).astype(F32), (b > 0).astype(F32))
        for c in range(4):
            from_left = jnp.where(a == 0, mine_ref[c], theirs_ref[c])
            from_right = jnp.where(a == 0, theirs_ref[c], mine_ref[c])
            halo0 = jnp.where(low, from_right, from_left)
            halo1 = jnp.where(low, roll_half(from_right, lay), roll_half(from_left, lay))
            own_halo_ref[c] = jnp.where(keep > 0, jnp.where(a == 0, halo0, halo1), 0.0)
            prt_halo_ref[c] = jnp.where(keep > 0, jnp.where(a == 0, halo1, halo0), 0.0)
        pack_blocks((place_ref, other_ref), own_ref, own_halo_ref, prt_ref, prt_halo_ref, blocks, lay, False, range(2))

    return body


def kernel_pack_second(lay):
    def body(place_ref, other_ref, own_ref, prt_ref, own_halo_ref, prt_halo_ref, *outs):
        places = (place_ref, other_ref)
        pack_blocks(places, own_ref, own_halo_ref, prt_ref, prt_halo_ref, outs, lay, False, range(2, 4))

    return body


def move(target, *arrays):
    count = len(arrays)
    inward = target is pltpu.VMEM
    here, there = vmem(), pl.BlockSpec(memory_space=pl.ANY)

    def body(*refs):
        sources, targets, sems = refs[:count], refs[count : 2 * count], refs[2 * count]
        copies = [pltpu.make_async_copy(x, y, sems.at[i]) for i, (x, y) in enumerate(zip(sources, targets))]
        for copy in copies:
            copy.start()
        for copy in copies:
            copy.wait()

    return pl.pallas_call(
        body,
        out_shape=tuple(target(x.shape, x.dtype) for x in arrays),
        in_specs=[there if inward else here] * count,
        out_specs=tuple(here if inward else there for _ in arrays),
        scratch_shapes=[pltpu.SemaphoreType.DMA((count,))],
        compiler_params=pltpu.CompilerParams(vmem_limit_bytes=2 * 1024 * 1024),
    )(*[pltpu.with_memory_space_constraint(x, pltpu.HBM if inward else pltpu.VMEM) for x in arrays])


def series(z, first):
    terms = [(-1) ** i / math.factorial(2 * i + first) for i in range(8)]
    value = terms[-1]
    for term in terms[-2::-1]:
        value = value * z + term
    return value


def kernel_slab(phase_ref, slab_ref):
    y = 0.5 * phase_ref[...]
    z = y * y
    sine, cosine = series(z, 1) * y, series(z, 0)
    slab_ref[0] = 1.0 - 2.0 * sine * sine
    slab_ref[1] = 2.0 * sine * cosine


def kernel_probe(lay, home):
    def body(place_ref, light_ref, out_ref):
        a, _, p = where_am_i()
        k = jnp.clip(lay.window_of(p, a, home), 0, lay.slots - 1)
        down, along = ((place_ref[0, 0, i, k] + (lay.t - lay.m)) % lay.t for i in range(2))
        for c in range(2):
            out_ref[c] = pltpu.roll(pltpu.roll(light_ref[c], down, 0), along, 1)

    return body


def assemble(blocks, window_ref, lay):
    p = lax.axis_index("pos")
    for s in range(lay.n):
        start = pl.multiple_of((p ^ s) * lay.h, lay.h)
        for c in range(window_ref.shape[0]):
            window_ref[c, pl.ds(start, lay.h), :] = blocks[s][c]


def propagate(o1r, o1i, light_ref, slab_ref, tab):
    er, ei = cmul(light_ref[0], light_ref[1], o1r, o1i)
    sr, si = transform(er, ei, tab, False)
    sr, si = cmul(sr, si, slab_ref[0], slab_ref[1])
    return transform(sr, si, tab, True)


def live(count_ref, lay, home):
    a, _, p = where_am_i()
    k = lay.window_of(p, a, home)
    return (k >= 0) & (k < count_ref[0, 0])


def scatter(value, c, outs, lay):
    p = lax.axis_index("pos")
    for s in range(lay.n):
        outs[s][c] = value[pl.ds(pl.multiple_of((p ^ s) * lay.h, lay.h), lay.h), :]


def kernel_backward(lay):
    def body(count_ref, *refs):
        n = lay.n
        blocks, (between_ref, tab, meas_ref, moved_ref) = refs[:n], refs[n : n + 4]
        toward_ref, outs, window_ref, grad_ref = refs[n + 4], refs[n + 5 : 2 * n + 5], *refs[2 * n + 5 :]

        used = live(count_ref, lay, False)

        @pl.when(used)
        def _():
            assemble(blocks, window_ref, lay)
            br, bi = between_ref[0], between_ref[1]
            lr, li = cmul(br, bi, window_ref[0], window_ref[1])
            fr, fi = transform(lr, li, tab, False)
            seen = jnp.where(lax.axis_index("ty") == 0, meas_ref[0, 0, 0], moved_ref[0, 0, 0])
            keeping = 1.0 - seen / jnp.maximum(jnp.sqrt(fr * fr + fi * fi), magnitude_floor)
            kr, ki = transform(fr * keeping, fi * keeping, tab, True)
            toward_ref[0], toward_ref[1] = cmul(window_ref[0], -window_ref[1], kr, ki)
            grad_ref[0], grad_ref[1] = cmul(br, -bi, kr, ki)
            for c in range(2):
                scatter(grad_ref.at[c], c, outs, lay)

        @pl.when(jnp.logical_not(used))
        def _():
            for out in outs:
                out[...] = jnp.zeros(out.shape, F32)

    return body


def kernel_final(lay):
    def body(count_ref, toward_ref, light_ref, slab_ref, tab, *refs):
        outs, grad_ref = refs[: lay.n], refs[lay.n]
        used = live(count_ref, lay, False)

        @pl.when(used)
        def _():
            sr, si = transform(toward_ref[0], toward_ref[1], tab, False)
            sr, si = cmul(sr, si, slab_ref[0], -slab_ref[1])
            ir, ii = transform(sr, si, tab, True)
            grad_ref[0], grad_ref[1] = cmul(light_ref[0], -light_ref[1], ir, ii)
            for c in range(2):
                scatter(grad_ref.at[c], c, outs, lay)

        @pl.when(jnp.logical_not(used))
        def _():
            for out in outs:
                out[...] = jnp.zeros(out.shape, F32)

    return body


def kernel_collect(lay):
    t, m = lay.t, lay.m

    def body(place_ref, other_ref, *refs):
        n = lay.n
        blocks, mom_ref = refs[: 2 * n], refs[2 * n]
        own_ref, halo_ref = refs[2 * n + 1 :]
        a, _, p = where_am_i()
        low = iota((lay.h, 2 * m), 1) < m
        own_ref[0] = momentum_rate * mom_ref[...]
        own_ref[1] = jnp.zeros(own_ref.shape[1:], F32)
        halo_ref[...] = jnp.zeros(halo_ref.shape, F32)
        for s in range(n):
            crosses = lay.crosses(s, False)
            row = 1 - a if crosses else a
            k = lay.window_of(p ^ s, row, False)
            valid = (k >= 0) & (k < lay.half)
            cells = lambda row=row, k=k: masks((place_ref, other_ref), row, k, p, lay, slice(0, lay.h))
            reaches = cells()[3]

            def add(i, rows, halo, s=s):
                inner, left, right = rows & ~halo, (rows & halo)[:, : 2 * m] & low, (rows & halo)[:, t - 2 * m :] & ~low
                for c in range(4):
                    g = blocks[c // 2 * n + s][c % 2]
                    own_ref[i, c] += jnp.where(inner, g, 0.0)
                    halo_ref[i, c] += jnp.where(left, g[:, : 2 * m], jnp.where(right, g[:, t - 2 * m :], 0.0))

            @pl.when(valid)
            def _(i=int(crosses), cells=cells, add=add):
                outside, _, halo, _ = cells()
                add(i, ~outside, halo)

            @pl.when(valid & reaches)
            def _(i=1 - int(crosses), cells=cells, add=add):
                _, partner, halo, _ = cells()
                add(i, partner, halo)

    return body


def kernel_strips_back(lay):
    t, m = lay.t, lay.m

    def body(own_ref, halo_ref, their_own_ref, their_halo_ref, sum_ref, halo_sum_ref, out_ref):
        a = lax.axis_index("ty")
        low = iota((lay.h, 2 * m), 1) < m
        for c in range(4):
            for i in range(2):
                sum_ref[i, c] = own_ref[i, c] + their_own_ref[1 - i, c]
                halo_sum_ref[i, c] = halo_ref[i, c] + their_halo_ref[1 - i, c]
        for row in (0, 1):

            @pl.when(a == row)
            def _(row=row):
                for tile in range(2):
                    i = tile ^ row
                    for c in range(4):
                        halo = halo_sum_ref[i, c]
                        if row == 0:
                            out_ref[tile, c] = jnp.where(low, halo, sum_ref[i, c, :, t - 2 * m :])
                        else:
                            out_ref[tile, c] = jnp.where(low, sum_ref[i, c, :, : 2 * m], halo)

    return body


def kernel_update(lay):
    m = lay.m

    def body(place_ref, obj_ref, prt_ref, obj_halo_ref, prt_halo_ref, sum_ref, halo_sum_ref, mine_ref, theirs_ref, *outs):
        n = lay.n
        new_ref, vel_ref, *blocks = outs[: 2 * n + 2]
        prt_new, own_halo, prt_halo = outs[2 * n + 2 :]
        a, b, _ = where_am_i()
        low = iota((lay.h, 2 * m), 1) < m
        not_first, not_last = b > 0, b < lay.ntx - 1
        keep = (low & not_last) | (~low & not_first)
        for i in range(2):
            tile = a if i == 0 else 1 - a
            for c in range(4):
                mine, theirs = mine_ref[tile, c], theirs_ref[tile, c]
                from_left = jnp.where(not_first, jnp.where(a == 0, mine, theirs), 0.0)
                from_right = jnp.where(not_last, jnp.where(a == 0, theirs, mine), 0.0)
                v = sum_ref[i, c] + jnp.concatenate(
                    [jnp.where(low, from_left, 0.0), jnp.where(low, 0.0, from_right)], axis=1
                )
                hv = halo_sum_ref[i, c] + jnp.where(low, from_right, from_left)
                obj, halo = (obj_ref, obj_halo_ref) if i == 0 else (prt_ref, prt_halo_ref)
                new, new_halo = (new_ref, own_halo) if i == 0 else (prt_new, prt_halo)
                if i == 0:
                    vel_ref[c] = v
                new[c] = obj[c] - step_length * v
                new_halo[c] = jnp.where(keep, halo[c] - step_length * hv, 0.0)
        pack_blocks((place_ref, place_ref), new_ref, own_halo, prt_new, prt_halo, blocks, lay, True, range(4))

    return body


def kernel_between(lay, home):
    def body(count_ref, *refs):
        n = lay.n
        blocks, (light_ref, slab_ref, tab), out_ref, window_ref = refs[:n], refs[n : n + 3], refs[n + 3], refs[n + 4]

        @pl.when(live(count_ref, lay, home))
        def _():
            assemble(blocks, window_ref, lay)
            out_ref[0], out_ref[1] = propagate(window_ref[0], window_ref[1], light_ref, slab_ref, tab)

    return body


def kernel_predict(lay):
    def body(count_ref, *refs):
        n = lay.n
        blocks, (between_ref, tab), out_ref, window_ref = refs[:n], refs[n : n + 2], refs[n + 2], refs[n + 3]
        used = live(count_ref, lay, True)

        @pl.when(used)
        def _():
            assemble(blocks, window_ref, lay)
            lr, li = cmul(between_ref[0], between_ref[1], window_ref[0], window_ref[1])
            fr, fi = transform(lr, li, tab, False)
            out_ref[0, 0, 0] = jnp.sqrt(fr * fr + fi * fi)

        @pl.when(jnp.logical_not(used))
        def _():
            out_ref[...] = jnp.zeros(out_ref.shape, F32)

    return body


def iteration(object_field, momentum, measured, illumination, slab_phase, offsets, entry_counts):
    lay = Layout(object_field, illumination, offsets)
    n, h, t, m = lay.n, lay.h, lay.t, lay.m
    own = object_field.reshape(4, h, t)
    offsets = offsets.transpose(0, 1, 3, 2)
    velocity_old = momentum.reshape(4, h, t)
    block, half_block, halo_shape = (4, h, t), (2, h, t), (4, h, 2 * m)
    tab = jnp.asarray(dft_tables(t))
    cores = lambda x: lax.ppermute(x, "ty", [(0, 1), (1, 0)])
    partner = cores(own)
    other_offsets = cores(offsets)
    (own,) = move(pltpu.VMEM, own)
    ntx = lay.ntx
    shift = [(b, b + 1) for b in range(ntx - 1)] + [(ntx - 1, 2 * ntx - 1)]
    shift += [(ntx + b + 1, ntx + b) for b in range(ntx - 1)] + [(ntx, 0)]
    columns = lambda x: lax.ppermute(x, ("ty", "tx"), shift)

    def exchange(values, pairs_of):
        got = [values[0]]
        for s in range(1, n):
            got.append(lax.ppermute(values[s], ("ty", "pos"), complete(pairs_of(s), n)))
        return got

    low, high = range(lay.half), range(lay.half, n)
    pairs = [(n + p, n + p + lay.half) for p in low] + [(p, p - lay.half) for p in high]
    pairs += [(p, n + p) for p in low] + [(n + p, p) for p in high]
    moved = lax.ppermute(measured, ("ty", "pos"), pairs)
    velocity_old, measured, illumination, slab_phase, tab = move(
        pltpu.VMEM, velocity_old, measured, illumination, slab_phase, tab
    )
    (slab,) = call(kernel_slab, [(2, t, t)], [slab_phase])
    lights = []
    for home in range(2):
        (light,) = call(kernel_probe(lay, bool(home)), [(2, t, t)], [offsets, illumination], 1)
        lights.append(light)
    light, light_home = lights
    (strips,) = call(kernel_strips(lay), [halo_shape], [own, partner])
    strips = columns(strips)
    strips_other = cores(strips)
    *blocks, own_halo, partner_halo = call(
        kernel_pack(lay),
        [half_block] * n + [halo_shape] * 2,
        [offsets, other_offsets, own, partner, strips, strips_other],
        2,
    )
    more = call(
        kernel_pack_second(lay), [half_block] * n, [offsets, other_offsets, own, partner, own_halo, partner_halo], 2
    )
    first = exchange(blocks, lambda s: lay.inward(s, False))
    second = exchange(more, lambda s: lay.inward(s, False))
    half_window = pltpu.VMEM((2, t, t), F32)

    def propagated(first, light, home):
        (between,) = call(
            kernel_between(lay, home), [(2, t, t)], [entry_counts, *first, light, slab, tab], 1, [half_window], limit=24
        )
        return between

    between = propagated(first, light, False)
    toward, *terms_second = call(
        kernel_backward(lay),
        [(2, t, t)] + [half_block] * n,
        [entry_counts, *second, between, tab, measured, moved],
        1,
        [half_window, half_window],
        limit=24,
    )
    parts_second = exchange(terms_second, lay.outward)
    terms_first = call(
        kernel_final(lay), [half_block] * n, [entry_counts, toward, light, slab, tab], 1, [half_window], limit=24
    )
    parts_first = exchange(terms_first, lay.outward)
    sums, halos = call(
        kernel_collect(lay),
        [(2, *block), (2, *halo_shape)],
        [offsets, other_offsets, *parts_first, *parts_second, velocity_old],
        2,
    )
    sums, halos, strips = call(
        kernel_strips_back(lay),
        [(2, *block), (2, *halo_shape), (2, *halo_shape)],
        [sums, halos, cores(sums), cores(halos)],
    )
    strips = columns(strips)
    updated, velocity, *rest = call(
        kernel_update(lay),
        [block] * 2 + [half_block] * (2 * n),
        [offsets, own, partner, own_halo, partner_halo, sums, halos, strips, cores(strips)],
        1,
        [pltpu.VMEM(block, F32), pltpu.VMEM(halo_shape, F32), pltpu.VMEM(halo_shape, F32)],
    )
    first = exchange(rest[:n], lambda s: lay.inward(s, True))
    second = exchange(rest[n : 2 * n], lambda s: lay.inward(s, True))
    updated, velocity = move(pltpu.HBM, updated, velocity)
    between = propagated(first, light_home, True)
    (amplitudes,) = call(
        kernel_predict(lay),
        [measured.shape],
        [entry_counts, *second, between, tab],
        1,
        [half_window],
        limit=24,
        last=True,
    )
    return (
        updated.reshape(object_field.shape),
        velocity.reshape(momentum.shape),
        amplitudes,
    )


def solution(mesh):
    placed = (
        P(None, None, ("ty", "pos"), "tx"),
        P(None, None, ("ty", "pos"), "tx"),
        P("ty", "tx", "pos", None, None),
        P(),
        P(),
        P("ty", "tx", None, None),
        P("ty", "tx"),
    )
    return jax.shard_map(
        iteration,
        mesh=mesh,
        in_specs=placed,
        out_specs=(
            P(None, None, ("ty", "pos"), "tx"),
            P(None, None, ("ty", "pos"), "tx"),
            P("ty", "tx", "pos", None, None),
        ),
        check_vma=False,
    )
```
